16 devices in a mesh: sp: 16 (over z, y, x, core).
Axes of the slice: x: 2, y: 2, z: 2, core: 2. Of those that a mesh axis runs over, the one named last changes fastest.
Arguments:
- x: bfloat16 [8, 2048, 2048], P(None, 'sp')
- d_y: bfloat16 [8, 2048, 2048], P(None, 'sp')
- ln_gamma: bfloat16 [2048], replicated
- ln_beta: bfloat16 [2048], replicated
- w_qkv: bfloat16 [2048, 6144], replicated
- b_qkv: bfloat16 [6144], replicated
- w_out: bfloat16 [2048, 2048], replicated
- b_out: bfloat16 [2048], replicated
- head_kind: int32 [16], replicated
Outputs:
- output 1: bfloat16 [8, 2048, 2048], P(None, 'sp')
- output 2: bfloat16 [8, 2048, 2048], P(None, 'sp')
- output 3: float32 [2048], replicated
- output 4: float32 [2048], replicated
- output 5: float32 [2048, 6144], replicated
- output 6: float32 [6144], replicated
- output 7: float32 [2048, 2048], replicated
- output 8: float32 [2048], replicated
All inputs are finite; a program needn't handle non-finite values.
Results may differ from the reference program's by a relative error of at most 0.0127672.
Values are sent between devices in bfloat16 or wider.
A program may use at most 1 GiB of HBM per device.

```python
import math
import jax
import jax.numpy as jnp
from jax import lax

BATCH_SIZE = 8
SEQ_LEN = 2048
D_MODEL = 2048
NUM_HEADS = 16
HEAD_DIM = D_MODEL // NUM_HEADS
BAND_WIDTH = SEQ_LEN // 4
QUERY_BLOCK = min(128, SEQ_LEN)
SCORE_SCALE = 1.0 / math.sqrt(HEAD_DIM)
LN_EPS = 1e-5
NEG_BIG = -1e30


def setup_inputs(seed: int = 0) -> dict:
    key_list = jax.random.split(jax.random.key(seed), 9)
    tok_shape = (BATCH_SIZE, SEQ_LEN, D_MODEL)
    w_scale = 1.0 / math.sqrt(D_MODEL)
    qkv_gain = jnp.array([1.7, 1.7, 1.0], jnp.float32)
    x_val = jax.random.normal(key_list[0], tok_shape, jnp.float32)
    dy_val = jax.random.normal(key_list[1], tok_shape, jnp.float32)
    gamma_val = 1.0 + 0.3 * jax.random.normal(key_list[2], (D_MODEL,), jnp.float32)
    beta_val = 0.3 * jax.random.normal(key_list[3], (D_MODEL,), jnp.float32)
    wqkv_val = jax.random.normal(key_list[4], (D_MODEL, 3, D_MODEL), jnp.float32) * qkv_gain[None, :, None] * w_scale
    bqkv_val = 0.5 * jax.random.normal(key_list[5], (3 * D_MODEL,), jnp.float32)
    wout_val = jax.random.normal(key_list[6], (D_MODEL, D_MODEL), jnp.float32) * w_scale
    bout_val = 0.5 * jax.random.normal(key_list[7], (D_MODEL,), jnp.float32)
    kind_val = (jax.random.permutation(key_list[8], NUM_HEADS) < NUM_HEADS // 2).astype(jnp.int32)
    return {
        "x": x_val.astype(jnp.bfloat16),
        "d_y": dy_val.astype(jnp.bfloat16),
        "ln_gamma": gamma_val.astype(jnp.bfloat16),
        "ln_beta": beta_val.astype(jnp.bfloat16),
        "w_qkv": wqkv_val.reshape(D_MODEL, 3 * D_MODEL).astype(jnp.bfloat16),
        "b_qkv": bqkv_val.astype(jnp.bfloat16),
        "w_out": wout_val.astype(jnp.bfloat16),
        "b_out": bout_val.astype(jnp.bfloat16),
        "head_kind": kind_val,
    }


def bf16_cast(values):
    return values.astype(jnp.bfloat16).astype(jnp.float32)


def layer_norm(x_rows, gamma_f, beta_f):
    row_mean = jnp.mean(x_rows, axis=-1, keepdims=True)
    centred = x_rows - row_mean
    row_var = jnp.mean(centred * centred, axis=-1, keepdims=True)
    return centred * lax.rsqrt(row_var + LN_EPS) * gamma_f + beta_f


def head_attention(q_head, k_head, v_head, banded):
    key_pos = jnp.arange(SEQ_LEN)[None, :]

    def query_block(q_start):
        q_part = lax.dynamic_slice_in_dim(q_head, q_start, QUERY_BLOCK, axis=1)
        logits = jnp.einsum("bqd,bkd->bqk", q_part, k_head) * SCORE_SCALE
        query_pos = q_start + jnp.arange(QUERY_BLOCK)[:, None]
        allowed = (key_pos <= query_pos) & ((banded == 0) | (key_pos > query_pos - BAND_WIDTH))
        attn_prob = jax.nn.softmax(jnp.where(allowed[None], logits, NEG_BIG), axis=-1)
        return bf16_cast(jnp.einsum("bqk,bkd->bqd", bf16_cast(attn_prob), v_head))

    return lax.map(jax.checkpoint(query_block), jnp.arange(SEQ_LEN // QUERY_BLOCK) * QUERY_BLOCK)


def block_forward(x_f, gamma_f, beta_f, wqkv_f, bqkv_f, wout_f, bout_f, head_kind):
    h_norm = bf16_cast(layer_norm(x_f, gamma_f, beta_f))
    qkv_tok = bf16_cast(jnp.dot(h_norm, wqkv_f, preferred_element_type=jnp.float32) + bqkv_f)
    qkv_head = jnp.transpose(qkv_tok.reshape(BATCH_SIZE, SEQ_LEN, 3, NUM_HEADS, HEAD_DIM), (2, 3, 0, 1, 4))

    def one_head(head_items):
        return head_attention(head_items[0], head_items[1], head_items[2], head_items[3])

    attn_heads = lax.map(one_head, (qkv_head[0], qkv_head[1], qkv_head[2], head_kind))
    attn_tok = jnp.transpose(attn_heads, (2, 1, 3, 0, 4)).reshape(BATCH_SIZE, SEQ_LEN, D_MODEL)
    return x_f + jnp.dot(attn_tok, wout_f, preferred_element_type=jnp.float32) + bout_f


def reference(x, d_y, ln_gamma, ln_beta, w_qkv, b_qkv, w_out, b_out, head_kind):
    def block_fn(x_f, gamma_f, beta_f, wqkv_f, bqkv_f, wout_f, bout_f):
        return block_forward(x_f, gamma_f, beta_f, wqkv_f, bqkv_f, wout_f, bout_f, head_kind)

    primal_list = [item_arr.astype(jnp.float32) for item_arr in (x, ln_gamma, ln_beta, w_qkv, b_qkv, w_out, b_out)]
    y_full, pull_back = jax.vjp(block_fn, *primal_list)
    grad_list = pull_back(d_y.astype(jnp.float32))
    return (y_full.astype(jnp.bfloat16), grad_list[0].astype(jnp.bfloat16), grad_list[1], grad_list[2], grad_list[3], grad_list[4], grad_list[5], grad_list[6])
```

```python
import functools
import math
import jax
import jax.numpy as jnp
from jax import lax
from jax.experimental import pallas as pl
from jax.experimental.pallas import tpu as pltpu
from jax.sharding import Mesh, PartitionSpec as P

LN_EPS = 1e-5
NEG_BIG = -1e30
LOG2_E = 1.4426950408889634


def layer_norm(x_rows, gamma_f, beta_f):
    row_mean = jnp.mean(x_rows, axis=-1, keepdims=True)
    centred = x_rows - row_mean
    row_var = jnp.mean(centred * centred, axis=-1, keepdims=True)
    return centred * lax.rsqrt(row_var + LN_EPS) * gamma_f + beta_f


def dot_nn(a, b):
    return lax.dot_general(a, b, (((1,), (0,)), ((), ())), preferred_element_type=jnp.float32)


def dot_nt(a, b):
    return lax.dot_general(a, b, (((1,), (1,)), ((), ())), preferred_element_type=jnp.float32)


def fold(x, op):
    return op(x.reshape(x.shape[0] // 8, 8, x.shape[1]), axis=0)


def attention_kernel(n_blk, half, kind_ref, core_ref, qa, ka, va, ga, qb, kb, vb, gb, oa, ob, dg,
                     qs, ks, vs, gs, kt, vt, s_scr, dp_scr, dk_scr, dv_scr, out_scr):
    head = pl.program_id(0)
    qi = pl.program_id(1)
    core = core_ref[0]
    blk = 2 * half
    scale = 1.0 / math.sqrt(qs.shape[2])
    at_a = pl.multiple_of(core * half, half)
    at_b = pl.multiple_of((1 - core) * half, half)

    @pl.when(qi == 0)
    def _():
        for dst, src_a, src_b in ((qs, qa, qb), (ks, ka, kb), (vs, va, vb), (gs, ga, gb)):
            for c in range(n_blk):
                dst[c, pl.ds(at_a, half), :] = src_a[c]
                dst[c, pl.ds(at_b, half), :] = src_b[c]
        for c in range(n_blk):
            kt[c] = jnp.transpose(ks[c])
            vt[c] = jnp.transpose(vs[c])
        dk_scr[...] = jnp.zeros_like(dk_scr)
        dv_scr[...] = jnp.zeros_like(dv_scr)

    def process(chunks, band_first):
        q = qs[qi]
        g = gs[qi]
        n = len(chunks)
        row = lax.broadcasted_iota(jnp.int32, (blk, blk), 0)
        col = lax.broadcasted_iota(jnp.int32, (blk, blk), 1)
        top = None
        for idx, c in enumerate(chunks):
            s = dot_nt(ks[c], q) * (scale * LOG2_E)
            if idx == n - 1:
                s = jnp.where(row <= col, s, NEG_BIG)
            if band_first and idx == 0:
                s = jnp.where(row > col, s, NEG_BIG)
            s_scr[idx] = s
            part = fold(s, jnp.max)
            top = part if top is None else jnp.maximum(top, part)
            dp_scr[idx] = dot_nt(vs[c], g).astype(jnp.bfloat16)
        top = jnp.max(top, axis=0, keepdims=True)
        total = None
        for idx in range(n):
            e = jnp.exp2(s_scr[idx] - top)
            s_scr[idx] = e
            part = fold(e, jnp.sum)
            total = part if total is None else total + part
        inv = 1.0 / jnp.sum(total, axis=0, keepdims=True)
        delta = None
        o_t = None
        for idx, c in enumerate(chunks):
            p = s_scr[idx] * inv
            s_scr[idx] = p
            part = fold(p * dp_scr[idx].astype(jnp.float32), jnp.sum)
            delta = part if delta is None else delta + part
            p_bf = p.astype(jnp.bfloat16)
            o_part = dot_nn(vt[c], p_bf)
            o_t = o_part if o_t is None else o_t + o_part
            dv_scr[c] += dot_nn(p_bf, g)
        delta = jnp.sum(delta, axis=0, keepdims=True)
        dq_t = None
        for idx, c in enumerate(chunks):
            ds = (s_scr[idx] * (dp_scr[idx].astype(jnp.float32) - delta)).astype(jnp.bfloat16)
            dq_part = dot_nn(kt[c], ds)
            dq_t = dq_part if dq_t is None else dq_t + dq_part
            dk_scr[c] += dot_nn(ds, q)
        out_scr[0] = jnp.transpose(o_t).astype(jnp.bfloat16)
        out_scr[1] = jnp.transpose(dq_t * scale).astype(jnp.bfloat16)

    banded = kind_ref[head] == 1
    for i in range(n_blk):
        cond = qi == i
        if i >= 2:
            cond = cond & jnp.logical_not(banded)

        @pl.when(cond)
        def _():
            process(list(range(i + 1)), False)

    @pl.when(banded & (qi >= 2))
    def _():
        process([qi - 2, qi - 1, qi], True)

    oa[qi] = out_scr[0, pl.ds(at_a, half), :]
    ob[qi] = out_scr[0, pl.ds(at_b, half), :]
    dg[0, 0, qi] = out_scr[1, pl.ds(at_a, half), :]
    dg[0, 1, qi] = out_scr[1, pl.ds(at_b, half), :]

    @pl.when(qi == n_blk - 1)
    def _():
        for c in range(n_blk):
            out_scr[0] = (dk_scr[c] * scale).astype(jnp.bfloat16)
            out_scr[1] = dv_scr[c].astype(jnp.bfloat16)
            dg[1, 0, c] = out_scr[0, pl.ds(at_a, half), :]
            dg[1, 1, c] = out_scr[0, pl.ds(at_b, half), :]
            dg[2, 0, c] = out_scr[1, pl.ds(at_a, half), :]
            dg[2, 1, c] = out_scr[1, pl.ds(at_b, half), :]


def attention(kinds, core, qkv_own, do_own, qkv_oth, do_oth):
    n_blk, half, _ = qkv_own.shape
    heads = kinds.shape[0]
    dim = 128
    blk = 2 * half

    def own(part):
        return pl.BlockSpec((n_blk, half, dim), lambda h, i, kind, cr: (0, 0, part * 2 * heads + cr[0] * heads + h))

    out3 = pl.BlockSpec((n_blk, half, dim), lambda h, i, kind, cr: (0, 0, h))
    out5 = pl.BlockSpec((3, 2, n_blk, half, dim), lambda h, i, kind, cr: (0, 0, 0, 0, h))
    bf = jnp.bfloat16
    wide = heads * dim
    flops = 6 * 2 * heads * (n_blk * blk) ** 2 * dim // 2
    return pl.pallas_call(
        functools.partial(attention_kernel, n_blk, half),
        grid_spec=pltpu.PrefetchScalarGridSpec(
            num_scalar_prefetch=2,
            grid=(heads, n_blk),
            in_specs=[own(0), own(1), own(2), own(0), out3, out3, out3, out3],
            out_specs=[out3, out3, out5],
            scratch_shapes=[pltpu.VMEM((n_blk, blk, dim), bf)] * 4
            + [pltpu.VMEM((n_blk, dim, blk), bf)] * 2
            + [pltpu.VMEM((n_blk, blk, blk), jnp.float32), pltpu.VMEM((n_blk, blk, blk), bf)]
            + [pltpu.VMEM((n_blk, blk, dim), jnp.float32)] * 2
            + [pltpu.VMEM((2, blk, dim), bf)],
        ),
        out_shape=[jax.ShapeDtypeStruct((n_blk, half, wide), bf)] * 2
        + [jax.ShapeDtypeStruct((3, 2, n_blk, half, wide), bf)],
        compiler_params=pltpu.CompilerParams(
            dimension_semantics=("arbitrary", "arbitrary"), vmem_limit_bytes=48 * 1024 * 1024
        ),
        cost_estimate=pl.CostEstimate(flops=flops, bytes_accessed=40 * 2**20, transcendentals=heads * (n_blk * blk) ** 2 // 2),
        name="attention_fwd_bwd",
    )(kinds, core, qkv_own, qkv_own, qkv_own, do_own, *qkv_oth, do_oth)


def copy_kernel(*refs):
    refs[-1][...] = refs[-2][...]


def place(piece, total_rows, first_row, dst=None):
    rows, cols = piece.shape
    tile = 128 if cols > 4096 else 512
    skip = first_row // tile
    in_specs = [pl.BlockSpec((tile, cols), lambda r: (r, 0))]
    args = [piece]
    aliases = {}
    if dst is not None:
        in_specs = [pl.BlockSpec(memory_space=pl.ANY)] + in_specs
        args = [dst] + args
        aliases = {0: 0}
    return pl.pallas_call(
        copy_kernel,
        grid=(rows // tile,),
        in_specs=in_specs,
        out_specs=pl.BlockSpec((tile, cols), lambda r: (r + skip, 0)),
        out_shape=jax.ShapeDtypeStruct((total_rows, cols), piece.dtype),
        input_output_aliases=aliases,
        cost_estimate=pl.CostEstimate(flops=rows * cols * 8, bytes_accessed=2 * piece.nbytes, transcendentals=0),
        name="place_rows",
    )(*args)


def grad_sum_kernel(n_chip, rows, g0, g1, g2, small, out, small_out, acc, rc, rb, ra, slots, load_sem, loc_sem,
                    c_send, c_recv, b_send, b_recv, a_send, a_recv, g_send, g_recv, s_send, s_recv, v_send, v_recv):
    chip = lax.axis_index("chip")
    core = lax.axis_index("core")
    n_dev = 2 * n_chip
    me = chip * 2 + core
    bits = [chip % 2, (chip // 2) % 2, chip // 4]
    beside = [chip + (1 - 2 * bits[d]) * (1 << d) for d in range(3)]
    parts = (g0, g1, g2)
    chunk = rows // 8
    wide = acc.shape[2]
    mesh_id = pl.DeviceIdType.MESH

    barrier = pltpu.get_barrier_semaphore()
    for o in range(1, n_dev):
        to = (me + o) % n_dev
        pl.semaphore_signal(barrier, inc=1, device_id=(to // 2, to % 2), device_id_type=mesh_id)
    pl.semaphore_wait(barrier, n_dev - 1)

    def flip(b, f):
        return 1 - b if f else b

    def remote(src, dst, send, recv, to_chip, to_core):
        c = pltpu.make_async_remote_copy(src_ref=src, dst_ref=dst, send_sem=send, recv_sem=recv,
                                         device_id=(to_chip, to_core), device_id_type=mesh_id)
        c.start()
        return c

    bc = [bits[t % 3] for t in range(3)]
    bb = [bits[(t + 1) % 3] for t in range(3)]
    ba = [bits[(t + 2) % 3] for t in range(3)]
    to_c = [beside[t % 3] for t in range(3)]
    to_b = [beside[(t + 1) % 3] for t in range(3)]
    to_a = [beside[(t + 2) % 3] for t in range(3)]

    def near(t, fb, fa):
        return pl.multiple_of(flip(bb[t], fb) * (2 * chunk) + flip(ba[t], fa) * chunk, chunk)

    def full(t, fc, fb, fa):
        return pl.multiple_of(flip(bc[t], fc) * (4 * chunk) + flip(bb[t], fb) * (2 * chunk) + flip(ba[t], fa) * chunk, chunk)

    flips = ((1, 1), (1, 0), (0, 1), (0, 0))
    c_copy = {}
    for j, (fb, fa) in enumerate(flips):
        for t in range(3):
            c_copy[t, j] = remote(parts[t].at[pl.ds(full(t, 1, fb, fa), chunk), :], rc.at[t, j],
                                  c_send.at[t, j], c_recv.at[t, j], to_c[t], core)
    loads = []
    for t in range(3):
        half_row = pl.multiple_of(bc[t] * (4 * chunk), 4 * chunk)
        load = pltpu.make_async_copy(parts[t].at[pl.ds(half_row, 4 * chunk), :], acc.at[t], load_sem.at[t])
        load.start()
        loads.append(load)
    v_copy = []
    for o in range(1, n_dev):
        to = (me + o) % n_dev
        v_copy.append(remote(small, slots.at[o], v_send.at[o], v_recv.at[o], to // 2, to % 2))
    slots[0] = small[...]
    for load in loads:
        load.wait()

    tile = 64

    def add(t, fb, fa, got):
        first = near(t, fb, fa)

        def step(i, carry):
            at = pl.ds(pl.multiple_of(first + i * tile, tile), tile)
            acc[t, at, :] = acc[t, at, :] + got[pl.ds(pl.multiple_of(i * tile, tile), tile), :]
            return carry

        lax.fori_loop(0, chunk // tile, step, 0)

    def held(t, fb, fa):
        return acc.at[t, pl.ds(near(t, fb, fa), chunk), :]

    b_copy = {}
    for j in range(2):
        fb, fa = flips[j]
        for t in range(3):
            c_copy[t, j].wait_recv()
            add(t, fb, fa, rc.at[t, j])
        for t in range(3):
            b_copy[t, j] = remote(held(t, fb, fa), rb.at[t, j], b_send.at[t, j], b_recv.at[t, j], to_b[t], core)
    for j in range(2, 4):
        fb, fa = flips[j]
        for t in range(3):
            c_copy[t, j].wait_recv()
            add(t, fb, fa, rc.at[t, j])
    a_copy = {}
    for t in range(3):
        b_copy[t, 0].wait_recv()
        add(t, 0, 1, rb.at[t, 0])
    for t in range(3):
        a_copy[t] = remote(held(t, 0, 1), ra.at[t], a_send.at[t], a_recv.at[t], to_a[t], core)
    for t in range(3):
        b_copy[t, 1].wait_recv()
        add(t, 0, 0, rb.at[t, 1])
    for t in range(3):
        a_copy[t].wait_recv()
        add(t, 0, 0, ra.at[t])

    def place_at(t, fc, fb, fa):
        return out.at[pl.ds(full(t, fc, fb, fa), chunk), pl.ds(pl.multiple_of((2 * t + core) * wide, wide), wide)]

    g_copy, s_copy, stores = {}, {}, []

    def gather(t, idx, src, dst, to):
        g_copy[t, idx] = remote(src, dst, g_send.at[t, idx], g_recv.at[t, idx], to, core)

    def share(t, idx, src, dst):
        s_copy[t, idx] = remote(src, dst, s_send.at[t, idx], s_recv.at[t, idx], chip, 1 - core)

    for idx, to in ((0, to_a), (1, to_b), (3, to_c)):
        for t in range(3):
            gather(t, idx, held(t, 0, 0), place_at(t, 0, 0, 0), to[t])
    for t in range(3):
        share(t, 0, held(t, 0, 0), place_at(t, 0, 0, 0))
        store = pltpu.make_async_copy(held(t, 0, 0), place_at(t, 0, 0, 0), loc_sem.at[t])
        store.start()
        stores.append(store)
    got_flips = ((0, 0, 1), (0, 1, 0), (0, 1, 1), (1, 0, 0), (1, 0, 1), (1, 1, 0), (1, 1, 1))
    onward = {0: ((2, to_b), (4, to_c)), 1: ((5, to_c),), 2: ((6, to_c),)}
    for idx in (0, 1, 3, 2, 4, 5, 6):
        for t in range(3):
            g_copy[t, idx].wait_recv()
            where = place_at(t, *got_flips[idx])
            for nxt, to in onward.get(idx, ()):
                gather(t, nxt, where, where, to[t])
            share(t, idx + 1, where, where)

    for copy in v_copy:
        copy.wait_recv()
    total = slots[me % n_dev]
    for d in range(1, n_dev):
        total = total + slots[(me + n_dev - d) % n_dev]
    small_out[...] = total

    for group in (s_copy,):
        for copy in group.values():
            copy.wait_recv()
    for group in (c_copy, b_copy, a_copy, g_copy, s_copy):
        for copy in group.values():
            copy.wait_send()
    for copy in v_copy:
        copy.wait_send()
    for store in stores:
        store.wait()


def grad_sum(n_chip, g_parts, small):
    rows, wide = g_parts[0].shape
    chunk = rows // 8
    n_dev = 2 * n_chip
    f32 = jnp.float32
    dma = pltpu.SemaphoreType.DMA
    hbm = pl.BlockSpec(memory_space=pl.ANY)
    vmem = pl.BlockSpec(memory_space=pltpu.VMEM)
    return pl.pallas_call(
        functools.partial(grad_sum_kernel, n_chip, rows),
        in_specs=[hbm, hbm, hbm, vmem],
        out_specs=[hbm, vmem],
        out_shape=[jax.ShapeDtypeStruct((rows, 6 * wide), f32), jax.ShapeDtypeStruct(small.shape, f32)],
        scratch_shapes=[
            pltpu.VMEM((3, 4 * chunk, wide), f32), pltpu.VMEM((3, 4, chunk, wide), f32),
            pltpu.VMEM((3, 2, chunk, wide), f32), pltpu.VMEM((3, chunk, wide), f32),
            pltpu.VMEM((n_dev,) + small.shape, f32), dma((3,)), dma((3,)),
            dma((3, 4)), dma((3, 4)), dma((3, 2)), dma((3, 2)), dma((3,)), dma((3,)),
            dma((3, 7)), dma((3, 7)), dma((3, 8)), dma((3, 8)), dma((n_dev,)), dma((n_dev,)),
        ],
        compiler_params=pltpu.CompilerParams(collective_id=0, has_side_effects=True, vmem_limit_bytes=44 * 1024 * 1024),
        cost_estimate=pl.CostEstimate(flops=3 * 10**11, bytes_accessed=150 * 2**20, transcendentals=0),
        name="grad_sum",
    )(*g_parts, small)


def solution(mesh):
    n_dev = mesh.shape["sp"]
    n_chip = n_dev // 2
    grid_mesh = Mesh(mesh.devices.reshape(n_chip, 2), ("chip", "core"))
    tok_spec = P(None, ("chip", "core"), None)
    swap_pairs = [(0, 1), (1, 0)]

    def local_block(x, d_y, ln_gamma, ln_beta, w_qkv, b_qkv, w_out, b_out, head_kind):
        half = x.shape[1]
        d_model = x.shape[2]
        num_heads = head_kind.shape[0]
        own_heads = num_heads // 2
        wide = d_model // 2
        n_tok = n_chip * half
        f32, bf = jnp.float32, jnp.bfloat16
        core = lax.axis_index("core")
        core_arr = jnp.full((1,), core, jnp.int32)
        my_kinds = lax.dynamic_slice_in_dim(head_kind, core * own_heads, own_heads)

        def swap(v):
            return lax.ppermute(v, "core", swap_pairs)

        def other_half(v, part):
            lo = v[:, part * d_model:part * d_model + wide]
            hi = v[:, part * d_model + wide:(part + 1) * d_model]
            return jnp.where(core == 0, hi, lo).reshape(n_chip, half, wide)

        def by_core(mine, theirs):
            return jnp.where(core == 0, mine, theirs), jnp.where(core == 0, theirs, mine)

        x_b = lax.all_to_all(x, "chip", 0, 0, tiled=True).reshape(n_tok, d_model)
        g_b = lax.all_to_all(d_y, "chip", 0, 0, tiled=True).reshape(n_tok, d_model)

        x_f = x_b.astype(f32)
        h_f, ln_pull = jax.vjp(layer_norm, x_f, ln_gamma.astype(f32), ln_beta.astype(f32))
        h_norm = h_f.astype(bf)
        h_all = jnp.concatenate([h_norm, swap(h_norm)], axis=0)
        qkv = (dot_nn(h_norm, w_qkv) + b_qkv.astype(f32)).astype(bf)
        qkv_own = qkv.reshape(n_chip, half, 3 * d_model)
        qkv_oth = [swap(other_half(qkv, part)) for part in range(3)]
        d_attn = dot_nt(g_b, w_out).astype(bf)
        do_own = d_attn.reshape(n_chip, half, d_model)
        do_oth = swap(other_half(d_attn, 0))

        o_own, o_send, dg = attention(my_kinds, core_arr, qkv_own, do_own, qkv_oth, do_oth)
        o_recv = swap(o_send)
        dg_own = dg[:, 0]
        dg_recv = swap(dg[:, 1])

        o_lo, o_hi = by_core(o_own, o_recv)
        attn_tok = jnp.concatenate([o_lo.reshape(n_tok, wide), o_hi.reshape(n_tok, wide)], axis=1)
        d_wout = lax.dot_general(attn_tok, g_b, (((0,), (0,)), ((), ())), preferred_element_type=f32)
        d_wout, dg_own, dg_recv = lax.optimization_barrier((d_wout, dg_own, dg_recv))
        d_wout = lax.psum(d_wout, ("chip", "core"))
        y_b = (x_f + dot_nn(attn_tok, w_out) + b_out.astype(f32)).astype(bf)
        y_out = lax.all_to_all(y_b.reshape(n_chip, half, d_model), "chip", 0, 0, tiled=True)

        dg_lo, dg_hi = by_core(dg_own.reshape(3, n_tok, wide), dg_recv.reshape(3, n_tok, wide))
        d_qkv = jnp.concatenate([dg_lo[0], dg_hi[0], dg_lo[1], dg_hi[1], dg_lo[2], dg_hi[2]], axis=1)
        d_h = dot_nt(d_qkv, w_qkv).astype(bf).astype(f32)
        d_x_ln, d_gamma, d_beta = ln_pull(d_h)
        d_x_b = (g_b.astype(f32) + d_x_ln).astype(bf)
        d_x = lax.all_to_all(d_x_b.reshape(n_chip, half, d_model), "chip", 0, 0, tiled=True)
        d_bqkv = jnp.sum(d_qkv, axis=0, dtype=f32)
        d_bout = jnp.sum(g_b, axis=0, dtype=f32)

        dg_tok = dg.reshape(3, 2 * n_tok, wide)
        d_w = [lax.dot_general(h_all, dg_tok[t], (((0,), (0,)), ((), ())), preferred_element_type=f32) for t in range(3)]
        small = jnp.concatenate([d_gamma, d_beta, d_bqkv, d_bout]).reshape(-1, 128)
        d_wqkv, small = grad_sum(n_chip, d_w, small)
        d_wqkv = place(d_wqkv, d_model, 0)
        small = small.reshape(-1)
        d_gamma, d_beta, d_bqkv, d_bout = (small[:d_model], small[d_model:2 * d_model], small[2 * d_model:5 * d_model], small[5 * d_model:])
        d_wout = place(d_wout, d_model, 0)
        y_out = place(y_out.reshape(n_tok, d_model), n_tok, 0).reshape(n_chip, half, d_model)
        d_x = place(d_x.reshape(n_tok, d_model), n_tok, 0).reshape(n_chip, half, d_model)
        return y_out, d_x, d_gamma, d_beta, d_wqkv, d_bqkv, d_wout, d_bout

    return jax.shard_map(
        local_block, mesh=grid_mesh,
        in_specs=(tok_spec, tok_spec, P(), P(), P(), P(), P(), P(), P()),
        out_specs=(tok_spec, tok_spec, P(), P(), P(), P(), P(), P()), check_vma=False)
```

```python
import functools
import math
import jax
import jax.numpy as jnp
from jax import lax
from jax.experimental import pallas as pl
from jax.experimental.pallas import tpu as pltpu
from jax.sharding import Mesh, PartitionSpec as P

LN_EPS = 1e-5
NEG_BIG = -1e30
LOG2_E = 1.4426950408889634


def layer_norm(x_rows, gamma_f, beta_f):
    row_mean = jnp.mean(x_rows, axis=-1, keepdims=True)
    centred = x_rows - row_mean
    row_var = jnp.mean(centred * centred, axis=-1, keepdims=True)
    return centred * lax.rsqrt(row_var + LN_EPS) * gamma_f + beta_f


def dot_nn(a, b):
    return lax.dot_general(a, b, (((1,), (0,)), ((), ())), preferred_element_type=jnp.float32)


def dot_nt(a, b):
    return lax.dot_general(a, b, (((1,), (1,)), ((), ())), preferred_element_type=jnp.float32)


def fold(x, op):
    return op(x.reshape(x.shape[0] // 8, 8, x.shape[1]), axis=0)


def attention_kernel(n_blk, half, kind_ref, core_ref, qa, ka, va, ga, qb, kb, vb, gb, oa, ob, da, db, bias,
                     qs, ks, vs, gs, kt, vt, s_scr, dp_scr, dk_scr, dv_scr, out_scr):
    head = pl.program_id(0)
    qi = pl.program_id(1)
    core = core_ref[0]
    blk = 2 * half
    scale = 1.0 / math.sqrt(qs.shape[2])
    at_a = pl.multiple_of(core * half, half)
    at_b = pl.multiple_of((1 - core) * half, half)

    @pl.when(qi == 0)
    def _():
        for dst, src_a, src_b in ((qs, qa, qb), (ks, ka, kb), (vs, va, vb), (gs, ga, gb)):
            for c in range(n_blk):
                dst[c, pl.ds(at_a, half), :] = src_a[c]
                dst[c, pl.ds(at_b, half), :] = src_b[c]
        for c in range(n_blk):
            kt[c] = jnp.transpose(ks[c])
            vt[c] = jnp.transpose(vs[c])
        dk_scr[...] = jnp.zeros_like(dk_scr)
        bias[...] = jnp.zeros_like(bias)
        dv_scr[...] = jnp.zeros_like(dv_scr)

    def process(chunks, band_first):
        q = qs[qi]
        g = gs[qi]
        n = len(chunks)
        row = lax.broadcasted_iota(jnp.int32, (blk, blk), 0)
        col = lax.broadcasted_iota(jnp.int32, (blk, blk), 1)
        top = None
        for idx, c in enumerate(chunks):
            s = dot_nt(ks[c], q) * (scale * LOG2_E)
            if idx == n - 1:
                s = jnp.where(row <= col, s, NEG_BIG)
            if band_first and idx == 0:
                s = jnp.where(row > col, s, NEG_BIG)
            s_scr[idx] = s
            part = fold(s, jnp.max)
            top = part if top is None else jnp.maximum(top, part)
            dp_scr[idx] = dot_nt(vs[c], g).astype(jnp.bfloat16)
        top = jnp.max(top, axis=0, keepdims=True)
        total = None
        for idx in range(n):
            e = jnp.exp2(s_scr[idx] - top)
            s_scr[idx] = e
            part = fold(e, jnp.sum)
            total = part if total is None else total + part
        inv = 1.0 / jnp.sum(total, axis=0, keepdims=True)
        delta = None
        o_t = None
        for idx, c in enumerate(chunks):
            p = s_scr[idx] * inv
            s_scr[idx] = p
            part = fold(p * dp_scr[idx].astype(jnp.float32), jnp.sum)
            delta = part if delta is None else delta + part
            p_bf = p.astype(jnp.bfloat16)
            o_part = dot_nn(vt[c], p_bf)
            o_t = o_part if o_t is None else o_t + o_part
            dv_scr[c] += dot_nn(p_bf, g)
        delta = jnp.sum(delta, axis=0, keepdims=True)
        dq_t = None
        for idx, c in enumerate(chunks):
            ds = (s_scr[idx] * (dp_scr[idx].astype(jnp.float32) - delta)).astype(jnp.bfloat16)
            dq_part = dot_nn(kt[c], ds)
            dq_t = dq_part if dq_t is None else dq_t + dq_part
            dk_scr[c] += dot_nn(ds, q)
        out_scr[0] = jnp.transpose(o_t).astype(jnp.bfloat16)
        out_scr[1] = jnp.transpose(dq_t * scale).astype(jnp.bfloat16)

    banded = kind_ref[head] == 1
    for i in range(n_blk):
        cond = qi == i
        if i >= 2:
            cond = cond & jnp.logical_not(banded)

        @pl.when(cond)
        def _():
            process(list(range(i + 1)), False)

    @pl.when(banded & (qi >= 2))
    def _():
        process([qi - 2, qi - 1, qi], True)

    def add_bias(part, v):
        bias[part] += fold(v.astype(jnp.float32), jnp.sum)

    add_bias(0, out_scr[1])
    oa[qi] = out_scr[0, pl.ds(at_a, half), :]
    ob[qi] = out_scr[0, pl.ds(at_b, half), :]
    da[0, qi] = out_scr[1, pl.ds(at_a, half), :]
    db[0, qi] = out_scr[1, pl.ds(at_b, half), :]

    @pl.when(qi == n_blk - 1)
    def _():
        for c in range(n_blk):
            out_scr[0] = (dk_scr[c] * scale).astype(jnp.bfloat16)
            out_scr[1] = dv_scr[c].astype(jnp.bfloat16)
            add_bias(1, out_scr[0])
            add_bias(2, out_scr[1])
            da[1, c] = out_scr[0, pl.ds(at_a, half), :]
            db[1, c] = out_scr[0, pl.ds(at_b, half), :]
            da[2, c] = out_scr[1, pl.ds(at_a, half), :]
            db[2, c] = out_scr[1, pl.ds(at_b, half), :]


def attention(kinds, core, qkv_own, do_own, qkv_oth, do_oth):
    _, n_blk, half, wide = qkv_own.shape
    heads = kinds.shape[0]
    dim = wide // heads
    blk = 2 * half

    def part(t):
        return pl.BlockSpec((None, n_blk, half, dim), lambda h, i, kind, cr: (t, 0, 0, h))

    one = pl.BlockSpec((n_blk, half, dim), lambda h, i, kind, cr: (0, 0, h))
    three = pl.BlockSpec((3, n_blk, half, dim), lambda h, i, kind, cr: (0, 0, 0, h))
    sums = pl.BlockSpec((None, 3, 8, dim), lambda h, i, kind, cr: (h, 0, 0, 0))
    bf = jnp.bfloat16
    flops = 6 * 2 * heads * (n_blk * blk) ** 2 * dim // 2
    return pl.pallas_call(
        functools.partial(attention_kernel, n_blk, half),
        grid_spec=pltpu.PrefetchScalarGridSpec(
            num_scalar_prefetch=2,
            grid=(heads, n_blk),
            in_specs=[part(0), part(1), part(2), one, part(0), part(1), part(2), one],
            out_specs=[one, one, three, three, sums],
            scratch_shapes=[pltpu.VMEM((n_blk, blk, dim), bf)] * 4
            + [pltpu.VMEM((n_blk, dim, blk), bf)] * 2
            + [pltpu.VMEM((n_blk, blk, blk), jnp.float32), pltpu.VMEM((n_blk, blk, blk), bf)]
            + [pltpu.VMEM((n_blk, blk, dim), jnp.float32)] * 2
            + [pltpu.VMEM((2, blk, dim), bf)],
        ),
        out_shape=[jax.ShapeDtypeStruct((n_blk, half, wide), bf)] * 2
        + [jax.ShapeDtypeStruct((3, n_blk, half, wide), bf)] * 2
        + [jax.ShapeDtypeStruct((heads, 3, 8, dim), jnp.float32)],
        compiler_params=pltpu.CompilerParams(
            dimension_semantics=("arbitrary", "arbitrary"), vmem_limit_bytes=48 * 1024 * 1024
        ),
        cost_estimate=pl.CostEstimate(flops=flops, bytes_accessed=40 * 2**20, transcendentals=heads * (n_blk * blk) ** 2 // 2),
        name="attention_fwd_bwd",
    )(kinds, core, qkv_own, qkv_own, qkv_own, do_own, qkv_oth, qkv_oth, qkv_oth, do_oth)


def matmul_call(body, scalars, grid, ins, outs, out_shape, flops):
    args = [a for a, _ in ins]
    moved = sum(a.size * a.dtype.itemsize for a in args)
    return pl.pallas_call(
        body,
        grid_spec=pltpu.PrefetchScalarGridSpec(
            num_scalar_prefetch=len(scalars), grid=grid, in_specs=[spec for _, spec in ins], out_specs=outs),
        out_shape=out_shape,
        compiler_params=pltpu.CompilerParams(
            dimension_semantics=("arbitrary",) * len(grid), vmem_limit_bytes=56 * 1024 * 1024),
        cost_estimate=pl.CostEstimate(flops=flops, bytes_accessed=moved, transcendentals=0),
    )(*scalars, *args)


def project_qkv(h, w, bias, group):
    n_tok, d_model = h.shape
    wide = d_model // 2
    tile = wide // 2

    def body(g, h_ref, w_ref, b_ref, out):
        out[...] = (dot_nn(h_ref[...], w_ref[...]) + b_ref[...].astype(jnp.float32)).astype(jnp.bfloat16)

    def cols(t, j, g):
        return (0, t * 4 + g[0] * 2 + j)

    return matmul_call(
        body, [group], (3, 2),
        [(h, pl.BlockSpec((n_tok, d_model), lambda t, j, g: (0, 0))),
         (w, pl.BlockSpec((d_model, tile), cols)), (bias, pl.BlockSpec((1, tile), cols))],
        pl.BlockSpec((None, n_tok, tile), lambda t, j, g: (t, 0, j)),
        jax.ShapeDtypeStruct((3, n_tok, wide), jnp.bfloat16), 6 * n_tok * d_model * wide)


def project_do(dy, w, group):
    n_tok, d_model = dy.shape
    wide = d_model // 2
    tile = wide // 2

    def body(g, dy_ref, w_ref, out):
        out[...] = dot_nt(dy_ref[...], w_ref[...]).astype(jnp.bfloat16)

    return matmul_call(
        body, [group], (2,),
        [(dy, pl.BlockSpec((n_tok, d_model), lambda j, g: (0, 0))),
         (w, pl.BlockSpec((tile, d_model), lambda j, g: (g[0] * 2 + j, 0)))],
        pl.BlockSpec((n_tok, tile), lambda j, g: (0, j)),
        jax.ShapeDtypeStruct((n_tok, wide), jnp.bfloat16), 2 * n_tok * d_model * wide)


def out_weight_grad(o_own, o_oth, dy, core):
    n_tok, d_model = dy.shape
    wide = d_model // 2
    tile = wide // 2

    def body(c, own, oth, dy_ref, out):
        @pl.when(pl.program_id(0) == 0)
        def _():
            out[...] = dot_nn(jnp.transpose(own[...]), dy_ref[...])

        @pl.when(pl.program_id(0) == 1)
        def _():
            out[...] = dot_nn(jnp.transpose(oth[...]), dy_ref[...])

    return matmul_call(
        body, [core], (2, 2),
        [(o_own, pl.BlockSpec((n_tok, tile), lambda s, j, c: (0, j * (1 - s) + s))),
         (o_oth, pl.BlockSpec((n_tok, tile), lambda s, j, c: (0, j * s))),
         (dy, pl.BlockSpec((n_tok, d_model), lambda s, j, c: (0, 0)))],
        pl.BlockSpec((tile, d_model), lambda s, j, c: (((1 - s) * c[0] + s * (1 - c[0])) * 2 + j, 0)),
        jax.ShapeDtypeStruct((d_model, d_model), jnp.float32), 2 * n_tok * d_model * d_model)


def project_out(x, o_own, o_oth, w, bias, core):
    n_tok, d_model = x.shape
    wide = d_model // 2
    tile = d_model // 4

    def body(c, x_ref, own, oth, w_own, w_oth, b_ref, out):
        y = dot_nn(own[...], w_own[...]) + dot_nn(oth[...], w_oth[...])
        out[...] = (x_ref[...].astype(jnp.float32) + y + b_ref[...].astype(jnp.float32)).astype(jnp.bfloat16)

    whole = pl.BlockSpec((n_tok, wide), lambda j, c: (0, 0))
    return matmul_call(
        body, [core], (4,),
        [(x, pl.BlockSpec((n_tok, tile), lambda j, c: (0, j))), (o_own, whole), (o_oth, whole),
         (w, pl.BlockSpec((wide, tile), lambda j, c: (c[0], j))), (w, pl.BlockSpec((wide, tile), lambda j, c: (1 - c[0], j))),
         (bias, pl.BlockSpec((1, tile), lambda j, c: (0, j)))],
        pl.BlockSpec((n_tok, tile), lambda j, c: (0, j)),
        jax.ShapeDtypeStruct((n_tok, d_model), jnp.bfloat16), 2 * n_tok * d_model * d_model)


def hidden_grad(dg_own, dg_oth, w, core):
    _, n_tok, wide = dg_own.shape
    d_model = 2 * wide
    tile = d_model // 8

    def body(c, own, oth, *refs):
        out = refs[-1]
        total = None
        for t in range(3):
            for src, w_ref in ((own, refs[t]), (oth, refs[3 + t])):
                one = dot_nt(src[t], w_ref[...])
                total = one if total is None else total + one
        out[...] = total.astype(jnp.bfloat16)

    whole = pl.BlockSpec((3, n_tok, wide), lambda j, c: (0, 0, 0))

    def col(t, mine):
        return pl.BlockSpec((tile, wide), lambda j, c: (j, 2 * t + (c[0] if mine else 1 - c[0])))

    return matmul_call(
        body, [core], (8,),
        [(dg_own, whole), (dg_oth, whole)] + [(w, col(t, True)) for t in range(3)] + [(w, col(t, False)) for t in range(3)],
        pl.BlockSpec((n_tok, tile), lambda j, c: (0, j)),
        jax.ShapeDtypeStruct((n_tok, d_model), jnp.bfloat16), 12 * n_tok * wide * d_model)


def qkv_weight_grad(h_own, h_oth, dg_own, dg_oth):
    n_tok, d_model = h_own.shape
    wide = d_model // 2
    tile = d_model // 4

    def body(ha, hb, da, db, out):
        out[...] = dot_nn(jnp.transpose(ha[...]), da[...]) + dot_nn(jnp.transpose(hb[...]), db[...])

    h_spec = pl.BlockSpec((n_tok, tile), lambda t, i: (0, i))
    d_spec = pl.BlockSpec((None, n_tok, wide), lambda t, i: (t, 0, 0))
    return matmul_call(
        body, [], (3, 4),
        [(h_own, h_spec), (h_oth, h_spec), (dg_own, d_spec), (dg_oth, d_spec)],
        pl.BlockSpec((None, tile, wide), lambda t, i: (t, i, 0)),
        jax.ShapeDtypeStruct((3, d_model, wide), jnp.float32), 12 * n_tok * d_model * wide)


def copy_kernel(*refs):
    refs[-1][...] = refs[-2][...]


def place(piece, total_rows, first_row, dst=None):
    rows, cols = piece.shape
    tile = 128 if cols > 4096 else 512
    skip = first_row // tile
    in_specs = [pl.BlockSpec((tile, cols), lambda r: (r, 0))]
    args = [piece]
    aliases = {}
    if dst is not None:
        in_specs = [pl.BlockSpec(memory_space=pl.ANY)] + in_specs
        args = [dst] + args
        aliases = {0: 0}
    return pl.pallas_call(
        copy_kernel,
        grid=(rows // tile,),
        in_specs=in_specs,
        out_specs=pl.BlockSpec((tile, cols), lambda r: (r + skip, 0)),
        out_shape=jax.ShapeDtypeStruct((total_rows, cols), piece.dtype),
        input_output_aliases=aliases,
        cost_estimate=pl.CostEstimate(flops=rows * cols * 8, bytes_accessed=2 * piece.nbytes, transcendentals=0),
        name="place_rows",
    )(*args)


def grad_sum_kernel(n_chip, rows, g_all, small, out, small_out, acc, rc, rb, ra, slots, load_sem, loc_sem,
                    c_send, c_recv, b_send, b_recv, a_send, a_recv, g_send, g_recv, s_send, s_recv, v_send, v_recv):
    chip = lax.axis_index("chip")
    core = lax.axis_index("core")
    n_dev = 2 * n_chip
    me = chip * 2 + core
    bits = [chip % 2, (chip // 2) % 2, chip // 4]
    beside = [chip + (1 - 2 * bits[d]) * (1 << d) for d in range(3)]
    parts = [g_all.at[t] for t in range(3)]
    chunk = rows // 8
    wide = acc.shape[2]
    mesh_id = pl.DeviceIdType.MESH

    barrier = pltpu.get_barrier_semaphore()
    for o in range(1, n_dev):
        to = (me + o) % n_dev
        pl.semaphore_signal(barrier, inc=1, device_id=(to // 2, to % 2), device_id_type=mesh_id)
    pl.semaphore_wait(barrier, n_dev - 1)

    def flip(b, f):
        return 1 - b if f else b

    def remote(src, dst, send, recv, to_chip, to_core):
        c = pltpu.make_async_remote_copy(src_ref=src, dst_ref=dst, send_sem=send, recv_sem=recv,
                                         device_id=(to_chip, to_core), device_id_type=mesh_id)
        c.start()
        return c

    bc = [bits[t % 3] for t in range(3)]
    bb = [bits[(t + 1) % 3] for t in range(3)]
    ba = [bits[(t + 2) % 3] for t in range(3)]
    to_c = [beside[t % 3] for t in range(3)]
    to_b = [beside[(t + 1) % 3] for t in range(3)]
    to_a = [beside[(t + 2) % 3] for t in range(3)]

    def near(t, fb, fa):
        return pl.multiple_of(flip(bb[t], fb) * (2 * chunk) + flip(ba[t], fa) * chunk, chunk)

    def full(t, fc, fb, fa):
        return pl.multiple_of(flip(bc[t], fc) * (4 * chunk) + flip(bb[t], fb) * (2 * chunk) + flip(ba[t], fa) * chunk, chunk)

    flips = ((1, 1), (1, 0), (0, 1), (0, 0))
    c_copy = {}
    for j, (fb, fa) in enumerate(flips):
        for t in range(3):
            c_copy[t, j] = remote(parts[t].at[pl.ds(full(t, 1, fb, fa), chunk), :], rc.at[t, j],
                                  c_send.at[t, j], c_recv.at[t, j], to_c[t], core)
    loads = []
    for t in range(3):
        half_row = pl.multiple_of(bc[t] * (4 * chunk), 4 * chunk)
        load = pltpu.make_async_copy(parts[t].at[pl.ds(half_row, 4 * chunk), :], acc.at[t], load_sem.at[t])
        load.start()
        loads.append(load)
    v_copy = []
    for o in range(1, n_dev):
        to = (me + o) % n_dev
        v_copy.append(remote(small, slots.at[o], v_send.at[o], v_recv.at[o], to // 2, to % 2))
    slots[0] = small[...]
    for load in loads:
        load.wait()

    tile = 64

    def add(t, fb, fa, got):
        first = near(t, fb, fa)

        def step(i, carry):
            at = pl.ds(pl.multiple_of(first + i * tile, tile), tile)
            acc[t, at, :] = acc[t, at, :] + got[pl.ds(pl.multiple_of(i * tile, tile), tile), :]
            return carry

        lax.fori_loop(0, chunk // tile, step, 0)

    def held(t, fb, fa):
        return acc.at[t, pl.ds(near(t, fb, fa), chunk), :]

    b_copy = {}
    for j in range(2):
        fb, fa = flips[j]
        for t in range(3):
            c_copy[t, j].wait_recv()
            add(t, fb, fa, rc.at[t, j])
        for t in range(3):
            b_copy[t, j] = remote(held(t, fb, fa), rb.at[t, j], b_send.at[t, j], b_recv.at[t, j], to_b[t], core)
    for j in range(2, 4):
        fb, fa = flips[j]
        for t in range(3):
            c_copy[t, j].wait_recv()
            add(t, fb, fa, rc.at[t, j])
    a_copy = {}
    for t in range(3):
        b_copy[t, 0].wait_recv()
        add(t, 0, 1, rb.at[t, 0])
    for t in range(3):
        a_copy[t] = remote(held(t, 0, 1), ra.at[t], a_send.at[t], a_recv.at[t], to_a[t], core)
    for t in range(3):
        b_copy[t, 1].wait_recv()
        add(t, 0, 0, rb.at[t, 1])
    for t in range(3):
        a_copy[t].wait_recv()
        add(t, 0, 0, ra.at[t])

    def place_at(t, fc, fb, fa):
        return out.at[pl.ds(full(t, fc, fb, fa), chunk), pl.ds(pl.multiple_of((2 * t + core) * wide, wide), wide)]

    g_copy, s_copy, stores = {}, {}, []

    def gather(t, idx, src, dst, to):
        g_copy[t, idx] = remote(src, dst, g_send.at[t, idx], g_recv.at[t, idx], to, core)

    def share(t, idx, src, dst):
        s_copy[t, idx] = remote(src, dst, s_send.at[t, idx], s_recv.at[t, idx], chip, 1 - core)

    for idx, to in ((0, to_a), (1, to_b), (3, to_c)):
        for t in range(3):
            gather(t, idx, held(t, 0, 0), place_at(t, 0, 0, 0), to[t])
    for t in range(3):
        share(t, 0, held(t, 0, 0), place_at(t, 0, 0, 0))
        store = pltpu.make_async_copy(held(t, 0, 0), place_at(t, 0, 0, 0), loc_sem.at[t])
        store.start()
        stores.append(store)
    got_flips = ((0, 0, 1), (0, 1, 0), (0, 1, 1), (1, 0, 0), (1, 0, 1), (1, 1, 0), (1, 1, 1))
    onward = {0: ((2, to_b), (4, to_c)), 1: ((5, to_c),), 2: ((6, to_c),)}
    for idx in (0, 1, 3, 2, 4, 5, 6):
        for t in range(3):
            g_copy[t, idx].wait_recv()
            where = place_at(t, *got_flips[idx])
            for nxt, to in onward.get(idx, ()):
                gather(t, nxt, where, where, to[t])
            share(t, idx + 1, where, where)

    for copy in v_copy:
        copy.wait_recv()
    total = slots[me % n_dev]
    for d in range(1, n_dev):
        total = total + slots[(me + n_dev - d) % n_dev]
    small_out[...] = total

    for group in (s_copy,):
        for copy in group.values():
            copy.wait_recv()
    for group in (c_copy, b_copy, a_copy, g_copy, s_copy):
        for copy in group.values():
            copy.wait_send()
    for copy in v_copy:
        copy.wait_send()
    for store in stores:
        store.wait()


def grad_sum(n_chip, g_all, small):
    _, rows, wide = g_all.shape
    chunk = rows // 8
    n_dev = 2 * n_chip
    f32 = jnp.float32
    dma = pltpu.SemaphoreType.DMA
    hbm = pl.BlockSpec(memory_space=pl.ANY)
    vmem = pl.BlockSpec(memory_space=pltpu.VMEM)
    return pl.pallas_call(
        functools.partial(grad_sum_kernel, n_chip, rows),
        in_specs=[hbm, vmem],
        out_specs=[hbm, vmem],
        out_shape=[jax.ShapeDtypeStruct((rows, 6 * wide), f32), jax.ShapeDtypeStruct(small.shape, f32)],
        scratch_shapes=[
            pltpu.VMEM((3, 4 * chunk, wide), f32), pltpu.VMEM((3, 4, chunk, wide), f32),
            pltpu.VMEM((3, 2, chunk, wide), f32), pltpu.VMEM((3, chunk, wide), f32),
            pltpu.VMEM((n_dev,) + small.shape, f32), dma((3,)), dma((3,)),
            dma((3, 4)), dma((3, 4)), dma((3, 2)), dma((3, 2)), dma((3,)), dma((3,)),
            dma((3, 7)), dma((3, 7)), dma((3, 8)), dma((3, 8)), dma((n_dev,)), dma((n_dev,)),
        ],
        compiler_params=pltpu.CompilerParams(collective_id=0, has_side_effects=True, vmem_limit_bytes=44 * 1024 * 1024),
        cost_estimate=pl.CostEstimate(flops=3 * 10**11, bytes_accessed=150 * 2**20, transcendentals=0),
        name="grad_sum",
    )(g_all, small)


def solution(mesh):
    n_dev = mesh.shape["sp"]
    n_chip = n_dev // 2
    grid_mesh = Mesh(mesh.devices.reshape(n_chip, 2), ("chip", "core"))
    tok_spec = P(None, ("chip", "core"), None)
    swap_pairs = [(0, 1), (1, 0)]

    def local_block(x, d_y, ln_gamma, ln_beta, w_qkv, b_qkv, w_out, b_out, head_kind):
        half = x.shape[1]
        d_model = x.shape[2]
        num_heads = head_kind.shape[0]
        own_heads = num_heads // 2
        wide = d_model // 2
        n_tok = n_chip * half
        f32, bf = jnp.float32, jnp.bfloat16
        core = lax.axis_index("core")
        core_arr = jnp.full((1,), core, jnp.int32)
        my_kinds = lax.dynamic_slice_in_dim(head_kind, core * own_heads, own_heads)

        def swap(v):
            return lax.ppermute(v, "core", swap_pairs)

        x_b = lax.all_to_all(x, "chip", 0, 0, tiled=True).reshape(n_tok, d_model)
        g_b = lax.all_to_all(d_y, "chip", 0, 0, tiled=True).reshape(n_tok, d_model)

        other_arr = 1 - core_arr
        blocks = (3, n_chip, half, wide)

        x_f = x_b.astype(f32)
        h_f, ln_pull = jax.vjp(layer_norm, x_f, ln_gamma.astype(f32), ln_beta.astype(f32))
        h_norm = h_f.astype(bf)
        bias_row = b_qkv.reshape(1, 3 * d_model)
        qkv_send = project_qkv(h_norm, w_qkv, bias_row, other_arr)
        qkv_oth = swap(qkv_send)
        qkv_own = project_qkv(h_norm, w_qkv, bias_row, core_arr)
        g_b, qkv_own = lax.optimization_barrier((g_b, qkv_own))
        do_oth = swap(project_do(g_b, w_out, other_arr))
        do_own = project_do(g_b, w_out, core_arr)
        h_oth = swap(h_norm)

        o_own, o_send, dg_own, dg_send, bias_sums = attention(
            my_kinds, core_arr, qkv_own.reshape(blocks), do_own.reshape(blocks[1:]),
            qkv_oth.reshape(blocks), do_oth.reshape(blocks[1:]))
        o_oth = swap(o_send).reshape(n_tok, wide)
        dg_oth = swap(dg_send).reshape(3, n_tok, wide)
        o_own = o_own.reshape(n_tok, wide)
        dg_own = dg_own.reshape(3, n_tok, wide)
        dg_send = dg_send.reshape(3, n_tok, wide)

        d_wout = out_weight_grad(o_own, o_oth, g_b, core_arr)
        d_wout, dg_own, dg_oth = lax.optimization_barrier((d_wout, dg_own, dg_oth))
        d_wout = lax.psum(d_wout, ("chip", "core"))
        y_b = project_out(x_b, o_own, o_oth, w_out, b_out.reshape(1, d_model), core_arr)
        y_out = lax.all_to_all(y_b.reshape(n_chip, half, d_model), "chip", 0, 0, tiled=True)

        d_h = hidden_grad(dg_own, dg_oth, w_qkv, core_arr)
        d_h = d_h.astype(f32)
        d_x_ln, d_gamma, d_beta = ln_pull(d_h)
        d_x_b = (g_b.astype(f32) + d_x_ln).astype(bf)
        d_x = lax.all_to_all(d_x_b.reshape(n_chip, half, d_model), "chip", 0, 0, tiled=True)
        bias_mine = jnp.sum(bias_sums, axis=2).transpose(1, 0, 2).reshape(3, 1, wide)
        d_bqkv = jnp.where(lax.broadcasted_iota(jnp.int32, (3, 2, wide), 1) == core, bias_mine, 0.0).reshape(3 * d_model)
        d_bout = jnp.sum(g_b, axis=0, dtype=f32)

        d_w = qkv_weight_grad(h_norm, h_oth, dg_own, dg_send)
        small = jnp.concatenate([d_gamma, d_beta, d_bqkv, d_bout]).reshape(-1, 128)
        d_wqkv, small = grad_sum(n_chip, d_w, small)
        d_wqkv = place(d_wqkv, d_model, 0)
        small = small.reshape(-1)
        d_gamma, d_beta, d_bqkv, d_bout = (small[:d_model], small[d_model:2 * d_model], small[2 * d_model:5 * d_model], small[5 * d_model:])
        d_wout = place(d_wout, d_model, 0)
        y_out = place(y_out.reshape(n_tok, d_model), n_tok, 0).reshape(n_chip, half, d_model)
        d_x = place(d_x.reshape(n_tok, d_model), n_tok, 0).reshape(n_chip, half, d_model)
        return y_out, d_x, d_gamma, d_beta, d_wqkv, d_bqkv, d_wout, d_bout

    return jax.shard_map(
        local_block, mesh=grid_mesh,
        in_specs=(tok_spec, tok_spec, P(), P(), P(), P(), P(), P(), P()),
        out_specs=(tok_spec, tok_spec, P(), P(), P(), P(), P(), P()), check_vma=False)
```

```python
import functools
import math
import jax
import jax.numpy as jnp
from jax import lax
from jax.experimental import pallas as pl
from jax.experimental.pallas import tpu as pltpu
from jax.sharding import Mesh, PartitionSpec as P

LN_EPS = 1e-5
NEG_BIG = -1e30
LOG2_E = 1.4426950408889634


def layer_norm(x_rows, gamma_f, beta_f):
    row_mean = jnp.mean(x_rows, axis=-1, keepdims=True)
    centred = x_rows - row_mean
    row_var = jnp.mean(centred * centred, axis=-1, keepdims=True)
    return centred * lax.rsqrt(row_var + LN_EPS) * gamma_f + beta_f


def dot_nn(a, b):
    return lax.dot_general(a, b, (((1,), (0,)), ((), ())), preferred_element_type=jnp.float32)


def dot_nt(a, b):
    return lax.dot_general(a, b, (((1,), (1,)), ((), ())), preferred_element_type=jnp.float32)


def fold(x, op):
    return op(x.reshape(x.shape[0] // 8, 8, x.shape[1]), axis=0)


def merge_halves(n_blk, half, at_a, at_b, triples):
    for dst, src_a, src_b in triples:
        for c in range(n_blk):
            dst[c, pl.ds(at_a, half), :] = src_a[c]
            dst[c, pl.ds(at_b, half), :] = src_b[c]


def block_cases(n_blk, qi, banded, process):
    for i in range(n_blk):
        cond = qi == i
        if i >= 2:
            cond = cond & jnp.logical_not(banded)

        @pl.when(cond)
        def _():
            process(list(range(i + 1)), False)

    @pl.when(banded & (qi >= 2))
    def _():
        process([qi - 2, qi - 1, qi], True)


def masked_scores(k, q, factor, last, band_first):
    s = dot_nt(k, q) * factor
    if last or band_first:
        row = lax.broadcasted_iota(jnp.int32, s.shape, 0)
        col = lax.broadcasted_iota(jnp.int32, s.shape, 1)
        s = jnp.where(row <= col if last else row > col, s, NEG_BIG)
    return s


def plus(total, part):
    return part if total is None else total + part


def forward_kernel(n_blk, half, kind_ref, core_ref, qa, ka, va, qb, kb, vb, oa, ob, lse, qs, ks, vs, vt, s_scr, out_scr):
    qi = pl.program_id(1)
    core = core_ref[0]
    factor = LOG2_E / math.sqrt(qs.shape[2])
    at_a = pl.multiple_of(core * half, half)
    at_b = pl.multiple_of((1 - core) * half, half)

    @pl.when(qi == 0)
    def _():
        merge_halves(n_blk, half, at_a, at_b, ((qs, qa, qb), (ks, ka, kb), (vs, va, vb)))
        for c in range(n_blk):
            vt[c] = jnp.transpose(vs[c])

    def process(chunks, band_first):
        q = qs[qi]
        n = len(chunks)
        top = None
        for idx, c in enumerate(chunks):
            s = masked_scores(ks[c], q, factor, idx == n - 1, band_first and idx == 0)
            s_scr[idx] = s
            part = fold(s, jnp.max)
            top = part if top is None else jnp.maximum(top, part)
        top = jnp.max(top, axis=0, keepdims=True)
        total = None
        for idx in range(n):
            e = jnp.exp2(s_scr[idx] - top)
            s_scr[idx] = e
            total = plus(total, fold(e, jnp.sum))
        total = jnp.sum(total, axis=0, keepdims=True)
        inv = 1.0 / total
        o_t = None
        for idx, c in enumerate(chunks):
            p_bf = (s_scr[idx] * inv).astype(jnp.bfloat16)
            o_t = plus(o_t, dot_nn(vt[c], p_bf))
        out_scr[...] = jnp.transpose(o_t).astype(jnp.bfloat16)
        lse[qi] = jnp.broadcast_to(top + jnp.log2(total), lse.shape[1:])

    block_cases(n_blk, qi, kind_ref[pl.program_id(0)] == 1, process)
    oa[qi] = out_scr[pl.ds(at_a, half), :]
    ob[qi] = out_scr[pl.ds(at_b, half), :]


def backward_kernel(n_blk, half, kind_ref, core_ref, qa, ka, va, ga, qb, kb, vb, gb, lse, da, db, bias,
                    qs, ks, vs, gs, kt, p_scr, dp_scr, dk_scr, dv_scr, out_scr):
    qi = pl.program_id(1)
    core = core_ref[0]
    scale = 1.0 / math.sqrt(qs.shape[2])
    at_a = pl.multiple_of(core * half, half)
    at_b = pl.multiple_of((1 - core) * half, half)

    @pl.when(qi == 0)
    def _():
        merge_halves(n_blk, half, at_a, at_b, ((qs, qa, qb), (ks, ka, kb), (vs, va, vb), (gs, ga, gb)))
        for c in range(n_blk):
            kt[c] = jnp.transpose(ks[c])
        dk_scr[...] = jnp.zeros_like(dk_scr)
        dv_scr[...] = jnp.zeros_like(dv_scr)
        bias[...] = jnp.zeros_like(bias)

    def process(chunks, band_first):
        q = qs[qi]
        g = gs[qi]
        n = len(chunks)
        shift = lse[qi][0:1]
        delta = None
        for idx, c in enumerate(chunks):
            p = jnp.exp2(masked_scores(ks[c], q, scale * LOG2_E, idx == n - 1, band_first and idx == 0) - shift)
            p_scr[idx] = p
            dp = dot_nt(vs[c], g).astype(jnp.bfloat16)
            dp_scr[idx] = dp
            delta = plus(delta, fold(p * dp.astype(jnp.float32), jnp.sum))
            dv_scr[c] += dot_nn(p.astype(jnp.bfloat16), g)
        delta = jnp.sum(delta, axis=0, keepdims=True)
        dq_t = None
        for idx, c in enumerate(chunks):
            ds = (p_scr[idx] * (dp_scr[idx].astype(jnp.float32) - delta)).astype(jnp.bfloat16)
            dq_t = plus(dq_t, dot_nn(kt[c], ds))
            dk_scr[c] += dot_nn(ds, q)
        out_scr[0] = jnp.transpose(dq_t * scale).astype(jnp.bfloat16)

    block_cases(n_blk, qi, kind_ref[pl.program_id(0)] == 1, process)

    def give(part, c, slot):
        bias[part] += fold(out_scr[slot].astype(jnp.float32), jnp.sum)
        da[part, c] = out_scr[slot, pl.ds(at_a, half), :]
        db[part, c] = out_scr[slot, pl.ds(at_b, half), :]

    give(0, qi, 0)

    @pl.when(qi == n_blk - 1)
    def _():
        for c in range(n_blk):
            out_scr[0] = (dk_scr[c] * scale).astype(jnp.bfloat16)
            out_scr[1] = dv_scr[c].astype(jnp.bfloat16)
            give(1, c, 0)
            give(2, c, 1)


def head_specs(n_blk, half, dim):
    def part(t):
        return pl.BlockSpec((None, n_blk, half, dim), lambda h, i, kind, cr: (t, 0, 0, h))

    one = pl.BlockSpec((n_blk, half, dim), lambda h, i, kind, cr: (0, 0, h))
    three = pl.BlockSpec((3, n_blk, half, dim), lambda h, i, kind, cr: (0, 0, 0, h))
    lse = pl.BlockSpec((None, n_blk, 8, 2 * half), lambda h, i, kind, cr: (h, 0, 0, 0))
    sums = pl.BlockSpec((None, 3, 8, dim), lambda h, i, kind, cr: (h, 0, 0, 0))
    return part, one, three, lse, sums


def attention_call(body, kinds, core, args, in_specs, out_specs, out_shape, scratch, n_tok, products):
    heads = kinds.shape[0]
    return pl.pallas_call(
        body,
        grid_spec=pltpu.PrefetchScalarGridSpec(
            num_scalar_prefetch=2, grid=(heads, n_tok[0]), in_specs=in_specs, out_specs=out_specs, scratch_shapes=scratch),
        out_shape=out_shape,
        compiler_params=pltpu.CompilerParams(
            dimension_semantics=("arbitrary", "arbitrary"), vmem_limit_bytes=48 * 1024 * 1024),
        cost_estimate=pl.CostEstimate(
            flops=products * heads * (n_tok[0] * n_tok[1]) ** 2 * 128, bytes_accessed=24 * 2**20,
            transcendentals=heads * (n_tok[0] * n_tok[1]) ** 2 // 2),
    )(kinds, core, *args)


def attention_forward(kinds, core, qkv_own, qkv_oth):
    _, n_blk, half, wide = qkv_own.shape
    heads = kinds.shape[0]
    dim = wide // heads
    blk = 2 * half
    bf = jnp.bfloat16
    part, one, _, lse, _ = head_specs(n_blk, half, dim)
    return attention_call(
        functools.partial(forward_kernel, n_blk, half), kinds, core, [qkv_own] * 3 + [qkv_oth] * 3,
        [part(0), part(1), part(2)] * 2, [one, one, lse],
        [jax.ShapeDtypeStruct((n_blk, half, wide), bf)] * 2 + [jax.ShapeDtypeStruct((heads, n_blk, 8, blk), jnp.float32)],
        [pltpu.VMEM((n_blk, blk, dim), bf)] * 3 + [pltpu.VMEM((n_blk, dim, blk), bf)]
        + [pltpu.VMEM((n_blk, blk, blk), jnp.float32), pltpu.VMEM((blk, dim), bf)],
        (n_blk, blk), 2)


def attention_backward(kinds, core, qkv_own, do_own, qkv_oth, do_oth, lse_arr):
    _, n_blk, half, wide = qkv_own.shape
    heads = kinds.shape[0]
    dim = wide // heads
    blk = 2 * half
    bf = jnp.bfloat16
    part, one, three, lse, sums = head_specs(n_blk, half, dim)
    return attention_call(
        functools.partial(backward_kernel, n_blk, half), kinds, core,
        [qkv_own] * 3 + [do_own] + [qkv_oth] * 3 + [do_oth, lse_arr],
        [part(0), part(1), part(2), one] * 2 + [lse], [three, three, sums],
        [jax.ShapeDtypeStruct((3, n_blk, half, wide), bf)] * 2 + [jax.ShapeDtypeStruct((heads, 3, 8, dim), jnp.float32)],
        [pltpu.VMEM((n_blk, blk, dim), bf)] * 4 + [pltpu.VMEM((n_blk, dim, blk), bf)]
        + [pltpu.VMEM((n_blk, blk, blk), jnp.float32), pltpu.VMEM((n_blk, blk, blk), bf)]
        + [pltpu.VMEM((n_blk, blk, dim), jnp.float32)] * 2 + [pltpu.VMEM((2, blk, dim), bf)],
        (n_blk, blk), 5)


def matmul_call(body, scalars, grid, ins, outs, out_shape, flops):
    args = [a for a, _ in ins]
    moved = sum(a.size * a.dtype.itemsize for a in args)
    return pl.pallas_call(
        body,
        grid_spec=pltpu.PrefetchScalarGridSpec(
            num_scalar_prefetch=len(scalars), grid=grid, in_specs=[spec for _, spec in ins], out_specs=outs),
        out_shape=out_shape,
        compiler_params=pltpu.CompilerParams(
            dimension_semantics=("arbitrary",) * len(grid), vmem_limit_bytes=56 * 1024 * 1024),
        cost_estimate=pl.CostEstimate(flops=flops, bytes_accessed=moved, transcendentals=0),
    )(*scalars, *args)


def project_qkv(h, w, bias, group):
    n_tok, d_model = h.shape
    wide = d_model // 2
    tile = wide // 2

    def body(g, h_ref, w_ref, b_ref, out):
        out[...] = (dot_nn(h_ref[...], w_ref[...]) + b_ref[...].astype(jnp.float32)).astype(jnp.bfloat16)

    def cols(t, j, g):
        return (0, t * 4 + g[0] * 2 + j)

    return matmul_call(
        body, [group], (3, 2),
        [(h, pl.BlockSpec((n_tok, d_model), lambda t, j, g: (0, 0))),
         (w, pl.BlockSpec((d_model, tile), cols)), (bias, pl.BlockSpec((1, tile), cols))],
        pl.BlockSpec((None, n_tok, tile), lambda t, j, g: (t, 0, j)),
        jax.ShapeDtypeStruct((3, n_tok, wide), jnp.bfloat16), 6 * n_tok * d_model * wide)


def project_do(dy, w, group):
    n_tok, d_model = dy.shape
    wide = d_model // 2
    tile = wide // 2

    def body(g, dy_ref, w_ref, out):
        out[...] = dot_nt(dy_ref[...], w_ref[...]).astype(jnp.bfloat16)

    return matmul_call(
        body, [group], (2,),
        [(dy, pl.BlockSpec((n_tok, d_model), lambda j, g: (0, 0))),
         (w, pl.BlockSpec((tile, d_model), lambda j, g: (g[0] * 2 + j, 0)))],
        pl.BlockSpec((n_tok, tile), lambda j, g: (0, j)),
        jax.ShapeDtypeStruct((n_tok, wide), jnp.bfloat16), 2 * n_tok * d_model * wide)


def out_weight_grad(o_own, o_oth, dy, core):
    n_tok, d_model = dy.shape
    wide = d_model // 2
    tile = wide // 2

    def body(c, own, oth, dy_ref, out):
        @pl.when(pl.program_id(0) == 0)
        def _():
            out[...] = dot_nn(jnp.transpose(own[...]), dy_ref[...])

        @pl.when(pl.program_id(0) == 1)
        def _():
            out[...] = dot_nn(jnp.transpose(oth[...]), dy_ref[...])

    return matmul_call(
        body, [core], (2, 2),
        [(o_own, pl.BlockSpec((n_tok, tile), lambda s, j, c: (0, j * (1 - s) + s))),
         (o_oth, pl.BlockSpec((n_tok, tile), lambda s, j, c: (0, j * s))),
         (dy, pl.BlockSpec((n_tok, d_model), lambda s, j, c: (0, 0)))],
        pl.BlockSpec((tile, d_model), lambda s, j, c: (((1 - s) * c[0] + s * (1 - c[0])) * 2 + j, 0)),
        jax.ShapeDtypeStruct((d_model, d_model), jnp.float32), 2 * n_tok * d_model * d_model)


def project_out(x, o_own, o_oth, w, bias, core):
    n_tok, d_model = x.shape
    wide = d_model // 2
    tile = d_model // 4

    def body(c, x_ref, own, oth, w_own, w_oth, b_ref, out):
        y = dot_nn(own[...], w_own[...]) + dot_nn(oth[...], w_oth[...])
        out[...] = (x_ref[...].astype(jnp.float32) + y + b_ref[...].astype(jnp.float32)).astype(jnp.bfloat16)

    whole = pl.BlockSpec((n_tok, wide), lambda j, c: (0, 0))
    return matmul_call(
        body, [core], (4,),
        [(x, pl.BlockSpec((n_tok, tile), lambda j, c: (0, j))), (o_own, whole), (o_oth, whole),
         (w, pl.BlockSpec((wide, tile), lambda j, c: (c[0], j))), (w, pl.BlockSpec((wide, tile), lambda j, c: (1 - c[0], j))),
         (bias, pl.BlockSpec((1, tile), lambda j, c: (0, j)))],
        pl.BlockSpec((n_tok, tile), lambda j, c: (0, j)),
        jax.ShapeDtypeStruct((n_tok, d_model), jnp.bfloat16), 2 * n_tok * d_model * d_model)


def hidden_grad(dg_own, dg_oth, w, core):
    _, n_tok, wide = dg_own.shape
    d_model = 2 * wide
    tile = d_model // 8

    def body(c, own, oth, *refs):
        out = refs[-1]
        total = None
        for t in range(3):
            for src, w_ref in ((own, refs[t]), (oth, refs[3 + t])):
                one = dot_nt(src[t], w_ref[...])
                total = one if total is None else total + one
        out[...] = total.astype(jnp.bfloat16)

    whole = pl.BlockSpec((3, n_tok, wide), lambda j, c: (0, 0, 0))

    def col(t, mine):
        return pl.BlockSpec((tile, wide), lambda j, c: (j, 2 * t + (c[0] if mine else 1 - c[0])))

    return matmul_call(
        body, [core], (8,),
        [(dg_own, whole), (dg_oth, whole)] + [(w, col(t, True)) for t in range(3)] + [(w, col(t, False)) for t in range(3)],
        pl.BlockSpec((n_tok, tile), lambda j, c: (0, j)),
        jax.ShapeDtypeStruct((n_tok, d_model), jnp.bfloat16), 12 * n_tok * wide * d_model)


def qkv_weight_grad(h_own, h_oth, dg_own, dg_oth):
    n_tok, d_model = h_own.shape
    wide = d_model // 2
    tile = d_model // 4

    def body(ha, hb, da, db, out):
        out[...] = dot_nn(jnp.transpose(ha[...]), da[...]) + dot_nn(jnp.transpose(hb[...]), db[...])

    h_spec = pl.BlockSpec((n_tok, tile), lambda t, i: (0, i))
    d_spec = pl.BlockSpec((None, n_tok, wide), lambda t, i: (t, 0, 0))
    return matmul_call(
        body, [], (3, 4),
        [(h_own, h_spec), (h_oth, h_spec), (dg_own, d_spec), (dg_oth, d_spec)],
        pl.BlockSpec((None, tile, wide), lambda t, i: (t, i, 0)),
        jax.ShapeDtypeStruct((3, d_model, wide), jnp.float32), 12 * n_tok * d_model * wide)


def copy_kernel(*refs):
    refs[-1][...] = refs[-2][...]


def place(piece, total_rows, first_row, dst=None):
    rows, cols = piece.shape
    tile = 128 if cols > 4096 else 512
    skip = first_row // tile
    in_specs = [pl.BlockSpec((tile, cols), lambda r: (r, 0))]
    args = [piece]
    aliases = {}
    if dst is not None:
        in_specs = [pl.BlockSpec(memory_space=pl.ANY)] + in_specs
        args = [dst] + args
        aliases = {0: 0}
    return pl.pallas_call(
        copy_kernel,
        grid=(rows // tile,),
        in_specs=in_specs,
        out_specs=pl.BlockSpec((tile, cols), lambda r: (r + skip, 0)),
        out_shape=jax.ShapeDtypeStruct((total_rows, cols), piece.dtype),
        input_output_aliases=aliases,
        cost_estimate=pl.CostEstimate(flops=rows * cols * 8, bytes_accessed=2 * piece.nbytes, transcendentals=0),
        name="place_rows",
    )(*args)


def grad_sum_kernel(n_chip, rows, g_all, small, out, small_out, acc, rc, rb, ra, slots, load_sem, loc_sem,
                    c_send, c_recv, b_send, b_recv, a_send, a_recv, g_send, g_recv, s_send, s_recv, v_send, v_recv):
    chip = lax.axis_index("chip")
    core = lax.axis_index("core")
    n_dev = 2 * n_chip
    me = chip * 2 + core
    bits = [chip % 2, (chip // 2) % 2, chip // 4]
    beside = [chip + (1 - 2 * bits[d]) * (1 << d) for d in range(3)]
    parts = [g_all.at[t] for t in range(3)]
    chunk = rows // 8
    wide = acc.shape[2]
    mesh_id = pl.DeviceIdType.MESH

    barrier = pltpu.get_barrier_semaphore()
    for o in range(1, n_dev):
        to = (me + o) % n_dev
        pl.semaphore_signal(barrier, inc=1, device_id=(to // 2, to % 2), device_id_type=mesh_id)
    pl.semaphore_wait(barrier, n_dev - 1)

    def flip(b, f):
        return 1 - b if f else b

    def remote(src, dst, send, recv, to_chip, to_core):
        c = pltpu.make_async_remote_copy(src_ref=src, dst_ref=dst, send_sem=send, recv_sem=recv,
                                         device_id=(to_chip, to_core), device_id_type=mesh_id)
        c.start()
        return c

    bc = [bits[t % 3] for t in range(3)]
    bb = [bits[(t + 1) % 3] for t in range(3)]
    ba = [bits[(t + 2) % 3] for t in range(3)]
    to_c = [beside[t % 3] for t in range(3)]
    to_b = [beside[(t + 1) % 3] for t in range(3)]
    to_a = [beside[(t + 2) % 3] for t in range(3)]

    def near(t, fb, fa):
        return pl.multiple_of(flip(bb[t], fb) * (2 * chunk) + flip(ba[t], fa) * chunk, chunk)

    def full(t, fc, fb, fa):
        return pl.multiple_of(flip(bc[t], fc) * (4 * chunk) + flip(bb[t], fb) * (2 * chunk) + flip(ba[t], fa) * chunk, chunk)

    flips = ((1, 1), (1, 0), (0, 1), (0, 0))
    c_copy = {}
    for j, (fb, fa) in enumerate(flips):
        for t in range(3):
            c_copy[t, j] = remote(parts[t].at[pl.ds(full(t, 1, fb, fa), chunk), :], rc.at[t, j],
                                  c_send.at[t, j], c_recv.at[t, j], to_c[t], core)
    loads = []
    for t in range(3):
        half_row = pl.multiple_of(bc[t] * (4 * chunk), 4 * chunk)
        load = pltpu.make_async_copy(parts[t].at[pl.ds(half_row, 4 * chunk), :], acc.at[t], load_sem.at[t])
        load.start()
        loads.append(load)
    v_copy = []
    for o in range(1, n_dev):
        to = (me + o) % n_dev
        v_copy.append(remote(small, slots.at[o], v_send.at[o], v_recv.at[o], to // 2, to % 2))
    slots[0] = small[...]
    for load in loads:
        load.wait()

    tile = 64

    def add(t, fb, fa, got):
        first = near(t, fb, fa)

        def step(i, carry):
            at = pl.ds(pl.multiple_of(first + i * tile, tile), tile)
            acc[t, at, :] = acc[t, at, :] + got[pl.ds(pl.multiple_of(i * tile, tile), tile), :]
            return carry

        lax.fori_loop(0, chunk // tile, step, 0)

    def held(t, fb, fa):
        return acc.at[t, pl.ds(near(t, fb, fa), chunk), :]

    b_copy = {}
    for j in range(2):
        fb, fa = flips[j]
        for t in range(3):
            c_copy[t, j].wait_recv()
            add(t, fb, fa, rc.at[t, j])
        for t in range(3):
            b_copy[t, j] = remote(held(t, fb, fa), rb.at[t, j], b_send.at[t, j], b_recv.at[t, j], to_b[t], core)
    for j in range(2, 4):
        fb, fa = flips[j]
        for t in range(3):
            c_copy[t, j].wait_recv()
            add(t, fb, fa, rc.at[t, j])
    a_copy = {}
    for t in range(3):
        b_copy[t, 0].wait_recv()
        add(t, 0, 1, rb.at[t, 0])
    for t in range(3):
        a_copy[t] = remote(held(t, 0, 1), ra.at[t], a_send.at[t], a_recv.at[t], to_a[t], core)
    for t in range(3):
        b_copy[t, 1].wait_recv()
        add(t, 0, 0, rb.at[t, 1])
    for t in range(3):
        a_copy[t].wait_recv()
        add(t, 0, 0, ra.at[t])

    def place_at(t, fc, fb, fa):
        return out.at[pl.ds(full(t, fc, fb, fa), chunk), pl.ds(pl.multiple_of((2 * t + core) * wide, wide), wide)]

    g_copy, s_copy, stores = {}, {}, []

    def gather(t, idx, src, dst, to):
        g_copy[t, idx] = remote(src, dst, g_send.at[t, idx], g_recv.at[t, idx], to, core)

    def share(t, idx, src, dst):
        s_copy[t, idx] = remote(src, dst, s_send.at[t, idx], s_recv.at[t, idx], chip, 1 - core)

    for idx, to in ((0, to_a), (1, to_b), (3, to_c)):
        for t in range(3):
            gather(t, idx, held(t, 0, 0), place_at(t, 0, 0, 0), to[t])
    for t in range(3):
        share(t, 0, held(t, 0, 0), place_at(t, 0, 0, 0))
        store = pltpu.make_async_copy(held(t, 0, 0), place_at(t, 0, 0, 0), loc_sem.at[t])
        store.start()
        stores.append(store)
    got_flips = ((0, 0, 1), (0, 1, 0), (0, 1, 1), (1, 0, 0), (1, 0, 1), (1, 1, 0), (1, 1, 1))
    onward = {0: ((2, to_b), (4, to_c)), 1: ((5, to_c),), 2: ((6, to_c),)}
    for idx in (0, 1, 3, 2, 4, 5, 6):
        for t in range(3):
            g_copy[t, idx].wait_recv()
            where = place_at(t, *got_flips[idx])
            for nxt, to in onward.get(idx, ()):
                gather(t, nxt, where, where, to[t])
            share(t, idx + 1, where, where)

    for copy in v_copy:
        copy.wait_recv()
    total = slots[me % n_dev]
    for d in range(1, n_dev):
        total = total + slots[(me + n_dev - d) % n_dev]
    small_out[...] = total

    for group in (s_copy,):
        for copy in group.values():
            copy.wait_recv()
    for group in (c_copy, b_copy, a_copy, g_copy, s_copy):
        for copy in group.values():
            copy.wait_send()
    for copy in v_copy:
        copy.wait_send()
    for store in stores:
        store.wait()


def grad_sum(n_chip, g_all, small):
    _, rows, wide = g_all.shape
    chunk = rows // 8
    n_dev = 2 * n_chip
    f32 = jnp.float32
    dma = pltpu.SemaphoreType.DMA
    hbm = pl.BlockSpec(memory_space=pl.ANY)
    vmem = pl.BlockSpec(memory_space=pltpu.VMEM)
    return pl.pallas_call(
        functools.partial(grad_sum_kernel, n_chip, rows),
        in_specs=[hbm, vmem],
        out_specs=[hbm, vmem],
        out_shape=[jax.ShapeDtypeStruct((rows, 6 * wide), f32), jax.ShapeDtypeStruct(small.shape, f32)],
        scratch_shapes=[
            pltpu.VMEM((3, 4 * chunk, wide), f32), pltpu.VMEM((3, 4, chunk, wide), f32),
            pltpu.VMEM((3, 2, chunk, wide), f32), pltpu.VMEM((3, chunk, wide), f32),
            pltpu.VMEM((n_dev,) + small.shape, f32), dma((3,)), dma((3,)),
            dma((3, 4)), dma((3, 4)), dma((3, 2)), dma((3, 2)), dma((3,)), dma((3,)),
            dma((3, 7)), dma((3, 7)), dma((3, 8)), dma((3, 8)), dma((n_dev,)), dma((n_dev,)),
        ],
        compiler_params=pltpu.CompilerParams(collective_id=0, has_side_effects=True, vmem_limit_bytes=44 * 1024 * 1024),
        cost_estimate=pl.CostEstimate(flops=3 * 10**11, bytes_accessed=150 * 2**20, transcendentals=0),
        name="grad_sum",
    )(g_all, small)


def solution(mesh):
    n_dev = mesh.shape["sp"]
    n_chip = n_dev // 2
    grid_mesh = Mesh(mesh.devices.reshape(n_chip, 2), ("chip", "core"))
    tok_spec = P(None, ("chip", "core"), None)
    swap_pairs = [(0, 1), (1, 0)]

    def local_block(x, d_y, ln_gamma, ln_beta, w_qkv, b_qkv, w_out, b_out, head_kind):
        half = x.shape[1]
        d_model = x.shape[2]
        num_heads = head_kind.shape[0]
        own_heads = num_heads // 2
        wide = d_model // 2
        n_tok = n_chip * half
        f32, bf = jnp.float32, jnp.bfloat16
        core = lax.axis_index("core")
        core_arr = jnp.full((1,), core, jnp.int32)
        my_kinds = lax.dynamic_slice_in_dim(head_kind, core * own_heads, own_heads)

        def swap(v):
            return lax.ppermute(v, "core", swap_pairs)

        x_b = lax.all_to_all(x, "chip", 0, 0, tiled=True).reshape(n_tok, d_model)
        g_b = lax.all_to_all(d_y, "chip", 0, 0, tiled=True).reshape(n_tok, d_model)

        other_arr = 1 - core_arr
        blocks = (3, n_chip, half, wide)

        x_f = x_b.astype(f32)
        h_f, ln_pull = jax.vjp(layer_norm, x_f, ln_gamma.astype(f32), ln_beta.astype(f32))
        h_norm = h_f.astype(bf)
        bias_row = b_qkv.reshape(1, 3 * d_model)
        qkv_send = project_qkv(h_norm, w_qkv, bias_row, other_arr)
        qkv_oth = swap(qkv_send).reshape(blocks)
        qkv_own = project_qkv(h_norm, w_qkv, bias_row, core_arr).reshape(blocks)
        g_b, qkv_own = lax.optimization_barrier((g_b, qkv_own))
        o_own, o_send, lse = attention_forward(my_kinds, core_arr, qkv_own, qkv_oth)
        o_oth = swap(o_send).reshape(n_tok, wide)
        o_own = o_own.reshape(n_tok, wide)
        do_oth = swap(project_do(g_b, w_out, other_arr)).reshape(blocks[1:])
        do_own = project_do(g_b, w_out, core_arr).reshape(blocks[1:])
        h_oth = swap(h_norm)

        d_wout = out_weight_grad(o_own, o_oth, g_b, core_arr)
        y_b = project_out(x_b, o_own, o_oth, w_out, b_out.reshape(1, d_model), core_arr)
        d_wout, y_b, do_own, do_oth = lax.optimization_barrier((d_wout, y_b, do_own, do_oth))
        d_wout = lax.psum(d_wout, ("chip", "core"))
        y_out = lax.all_to_all(y_b.reshape(n_chip, half, d_model), "chip", 0, 0, tiled=True)

        dg_own, dg_send, bias_sums = attention_backward(my_kinds, core_arr, qkv_own, do_own, qkv_oth, do_oth, lse)
        dg_oth = swap(dg_send).reshape(3, n_tok, wide)
        dg_own = dg_own.reshape(3, n_tok, wide)
        dg_send = dg_send.reshape(3, n_tok, wide)

        d_h = hidden_grad(dg_own, dg_oth, w_qkv, core_arr).astype(f32)
        d_x_ln, d_gamma, d_beta = ln_pull(d_h)
        d_x_b = (g_b.astype(f32) + d_x_ln).astype(bf)
        d_x = lax.all_to_all(d_x_b.reshape(n_chip, half, d_model), "chip", 0, 0, tiled=True)
        bias_mine = jnp.sum(bias_sums, axis=2).transpose(1, 0, 2).reshape(3, 1, wide)
        d_bqkv = jnp.where(lax.broadcasted_iota(jnp.int32, (3, 2, wide), 1) == core, bias_mine, 0.0).reshape(3 * d_model)
        d_bout = jnp.sum(g_b, axis=0, dtype=f32)

        d_w = qkv_weight_grad(h_norm, h_oth, dg_own, dg_send)
        small = jnp.concatenate([d_gamma, d_beta, d_bqkv, d_bout]).reshape(-1, 128)
        d_wqkv, small = grad_sum(n_chip, d_w, small)
        d_wqkv = place(d_wqkv, d_model, 0)
        small = small.reshape(-1)
        d_gamma, d_beta, d_bqkv, d_bout = (small[:d_model], small[d_model:2 * d_model], small[2 * d_model:5 * d_model], small[5 * d_model:])
        d_wout = place(d_wout, d_model, 0)
        y_out = place(y_out.reshape(n_tok, d_model), n_tok, 0).reshape(n_chip, half, d_model)
        d_x = place(d_x.reshape(n_tok, d_model), n_tok, 0).reshape(n_chip, half, d_model)
        return y_out, d_x, d_gamma, d_beta, d_wqkv, d_bqkv, d_wout, d_bout

    return jax.shard_map(
        local_block, mesh=grid_mesh,
        in_specs=(tok_spec, tok_spec, P(), P(), P(), P(), P(), P(), P()),
        out_specs=(tok_spec, tok_spec, P(), P(), P(), P(), P(), P()), check_vma=False)
```

```python
import functools
import math
import jax
import jax.numpy as jnp
from jax import lax
from jax.experimental import pallas as pl
from jax.experimental.pallas import tpu as pltpu
from jax.sharding import Mesh, PartitionSpec as P

LN_EPS = 1e-5
NEG_BIG = -1e30
LOG2_E = 1.4426950408889634


def layer_norm(x_rows, gamma_f, beta_f):
    row_mean = jnp.mean(x_rows, axis=-1, keepdims=True)
    centred = x_rows - row_mean
    row_var = jnp.mean(centred * centred, axis=-1, keepdims=True)
    return centred * lax.rsqrt(row_var + LN_EPS) * gamma_f + beta_f


def dot_nn(a, b):
    return lax.dot_general(a, b, (((1,), (0,)), ((), ())), preferred_element_type=jnp.float32)


def dot_nt(a, b):
    return lax.dot_general(a, b, (((1,), (1,)), ((), ())), preferred_element_type=jnp.float32)


def fold(x, op):
    return op(x.reshape(x.shape[0] // 8, 8, x.shape[1]), axis=0)


def merge_halves(n_blk, half, at_a, at_b, triples):
    for dst, src_a, src_b in triples:
        for c in range(n_blk):
            dst[c, pl.ds(at_a, half), :] = src_a[c]
            dst[c, pl.ds(at_b, half), :] = src_b[c]


def block_cases(n_blk, pair, banded, process):
    for i in range(n_blk // 2):
        cond = pair == i
        if i >= 1:
            cond = cond & jnp.logical_not(banded)

        @pl.when(cond)
        def _():
            process(list(range(2 * i + 2)), ((0, 2 * i + 1), (0, 2 * i + 2)), False)

    @pl.when(banded & (pair >= 1))
    def _():
        process([2 * pair - 2 + i for i in range(4)], ((0, 3), (1, 4)), True)


def masked_scores(k, q, factor, last, band_first):
    s = dot_nt(k, q) * factor
    if last or band_first:
        row = lax.broadcasted_iota(jnp.int32, s.shape, 0)
        col = lax.broadcasted_iota(jnp.int32, s.shape, 1)
        s = jnp.where(row <= col if last else row > col, s, NEG_BIG)
    return s


def plus(total, part):
    return part if total is None else total + part


def forward_kernel(n_blk, half, kind_ref, core_ref, qa, ka, va, qb, kb, vb, oa, ob, lse, qs, ks, vs, vt, s_scr, out_scr):
    pair = pl.program_id(1)
    core = core_ref[0]
    factor = LOG2_E / math.sqrt(qs.shape[2])
    at_a = pl.multiple_of(core * half, half)
    at_b = pl.multiple_of((1 - core) * half, half)

    @pl.when(pair == 0)
    def _():
        merge_halves(n_blk, half, at_a, at_b, ((qs, qa, qb), (ks, ka, kb), (vs, va, vb)))
        for c in range(n_blk):
            vt[c] = jnp.transpose(vs[c])

    def process(chunks, ranges, banded):
        tops, sums = [None, None], [None, None]
        for idx, c in enumerate(chunks):
            for r, (lo, hi) in enumerate(ranges):
                if lo <= idx < hi:
                    s = masked_scores(ks[c], qs[2 * pair + r], factor, idx == hi - 1, banded and idx == lo)
                    s_scr[r, idx] = s
                    part = fold(s, jnp.max)
                    tops[r] = part if tops[r] is None else jnp.maximum(tops[r], part)
        for r, (lo, hi) in enumerate(ranges):
            tops[r] = jnp.max(tops[r], axis=0, keepdims=True)
            for idx in range(lo, hi):
                e = jnp.exp2(s_scr[r, idx] - tops[r])
                s_scr[r, idx] = e
                sums[r] = plus(sums[r], fold(e, jnp.sum))
        for r, (lo, hi) in enumerate(ranges):
            total = jnp.sum(sums[r], axis=0, keepdims=True)
            inv = 1.0 / total
            o_t = None
            for idx in range(lo, hi):
                o_t = plus(o_t, dot_nn(vt[chunks[idx]], (s_scr[r, idx] * inv).astype(jnp.bfloat16)))
            out_scr[r] = jnp.transpose(o_t).astype(jnp.bfloat16)
            lse[2 * pair + r] = jnp.broadcast_to(tops[r] + jnp.log2(total), lse.shape[1:])

    block_cases(n_blk, pair, kind_ref[pl.program_id(0)] == 1, process)
    for r in range(2):
        oa[2 * pair + r] = out_scr[r, pl.ds(at_a, half), :]
        ob[2 * pair + r] = out_scr[r, pl.ds(at_b, half), :]


def backward_kernel(n_blk, half, kind_ref, core_ref, qa, ka, va, ga, qb, kb, vb, gb, lse, da, db, bias,
                    qs, ks, vs, gs, kt, p_scr, dp_scr, dk_scr, dv_scr, out_scr):
    pair = pl.program_id(1)
    core = core_ref[0]
    scale = 1.0 / math.sqrt(qs.shape[2])
    at_a = pl.multiple_of(core * half, half)
    at_b = pl.multiple_of((1 - core) * half, half)

    @pl.when(pair == 0)
    def _():
        merge_halves(n_blk, half, at_a, at_b, ((qs, qa, qb), (ks, ka, kb), (vs, va, vb), (gs, ga, gb)))
        for c in range(n_blk):
            kt[c] = jnp.transpose(ks[c])
        dk_scr[...] = jnp.zeros_like(dk_scr)
        dv_scr[...] = jnp.zeros_like(dv_scr)
        bias[...] = jnp.zeros_like(bias)

    def process(chunks, ranges, banded):
        deltas, dq_t = [None, None], [None, None]
        for idx, c in enumerate(chunks):
            dv = None
            for r, (lo, hi) in enumerate(ranges):
                if lo <= idx < hi:
                    qi = 2 * pair + r
                    s = masked_scores(ks[c], qs[qi], scale * LOG2_E, idx == hi - 1, banded and idx == lo)
                    p = jnp.exp2(s - lse[qi][0:1])
                    p_scr[r, idx] = p
                    dp = dot_nt(vs[c], gs[qi]).astype(jnp.bfloat16)
                    dp_scr[r, idx] = dp
                    deltas[r] = plus(deltas[r], fold(p * dp.astype(jnp.float32), jnp.sum))
                    dv = plus(dv, dot_nn(p.astype(jnp.bfloat16), gs[qi]))
            dv_scr[c] += dv
        deltas = [jnp.sum(d, axis=0, keepdims=True) for d in deltas]
        for idx, c in enumerate(chunks):
            dk = None
            for r, (lo, hi) in enumerate(ranges):
                if lo <= idx < hi:
                    ds = (p_scr[r, idx] * (dp_scr[r, idx].astype(jnp.float32) - deltas[r])).astype(jnp.bfloat16)
                    dq_t[r] = plus(dq_t[r], dot_nn(kt[c], ds))
                    dk = plus(dk, dot_nn(ds, qs[2 * pair + r]))
            dk_scr[c] += dk
        for r in range(2):
            out_scr[r] = jnp.transpose(dq_t[r] * scale).astype(jnp.bfloat16)

    block_cases(n_blk, pair, kind_ref[pl.program_id(0)] == 1, process)

    def give(part, c, slot):
        bias[part] += fold(out_scr[slot].astype(jnp.float32), jnp.sum)
        da[part, c] = out_scr[slot, pl.ds(at_a, half), :]
        db[part, c] = out_scr[slot, pl.ds(at_b, half), :]

    for r in range(2):
        give(0, 2 * pair + r, r)

    @pl.when(pair == n_blk // 2 - 1)
    def _():
        for c in range(n_blk):
            out_scr[0] = (dk_scr[c] * scale).astype(jnp.bfloat16)
            out_scr[1] = dv_scr[c].astype(jnp.bfloat16)
            give(1, c, 0)
            give(2, c, 1)


def head_specs(n_blk, half, dim):
    def part(t):
        return pl.BlockSpec((None, n_blk, half, dim), lambda h, i, kind, cr: (t, 0, 0, h))

    one = pl.BlockSpec((n_blk, half, dim), lambda h, i, kind, cr: (0, 0, h))
    three = pl.BlockSpec((3, n_blk, half, dim), lambda h, i, kind, cr: (0, 0, 0, h))
    lse = pl.BlockSpec((None, n_blk, 8, 2 * half), lambda h, i, kind, cr: (h, 0, 0, 0))
    sums = pl.BlockSpec((None, 3, 8, dim), lambda h, i, kind, cr: (h, 0, 0, 0))
    return part, one, three, lse, sums


def attention_call(body, kinds, core, args, in_specs, out_specs, out_shape, scratch, n_tok, products):
    heads = kinds.shape[0]
    return pl.pallas_call(
        body,
        grid_spec=pltpu.PrefetchScalarGridSpec(
            num_scalar_prefetch=2, grid=(heads, n_tok[0] // 2), in_specs=in_specs, out_specs=out_specs, scratch_shapes=scratch),
        out_shape=out_shape,
        compiler_params=pltpu.CompilerParams(
            dimension_semantics=("arbitrary", "arbitrary"), vmem_limit_bytes=48 * 1024 * 1024),
        cost_estimate=pl.CostEstimate(
            flops=products * heads * (n_tok[0] * n_tok[1]) ** 2 * 128, bytes_accessed=24 * 2**20,
            transcendentals=heads * (n_tok[0] * n_tok[1]) ** 2 // 2),
    )(kinds, core, *args)


def attention_forward(kinds, core, qkv_own, qkv_oth):
    _, n_blk, half, wide = qkv_own.shape
    heads = kinds.shape[0]
    dim = wide // heads
    blk = 2 * half
    bf = jnp.bfloat16
    part, one, _, lse, _ = head_specs(n_blk, half, dim)
    return attention_call(
        functools.partial(forward_kernel, n_blk, half), kinds, core, [qkv_own] * 3 + [qkv_oth] * 3,
        [part(0), part(1), part(2)] * 2, [one, one, lse],
        [jax.ShapeDtypeStruct((n_blk, half, wide), bf)] * 2 + [jax.ShapeDtypeStruct((heads, n_blk, 8, blk), jnp.float32)],
        [pltpu.VMEM((n_blk, blk, dim), bf)] * 3 + [pltpu.VMEM((n_blk, dim, blk), bf)]
        + [pltpu.VMEM((2, n_blk, blk, blk), jnp.float32), pltpu.VMEM((2, blk, dim), bf)],
        (n_blk, blk), 2)


def attention_backward(kinds, core, qkv_own, do_own, qkv_oth, do_oth, lse_arr):
    _, n_blk, half, wide = qkv_own.shape
    heads = kinds.shape[0]
    dim = wide // heads
    blk = 2 * half
    bf = jnp.bfloat16
    part, one, three, lse, sums = head_specs(n_blk, half, dim)
    return attention_call(
        functools.partial(backward_kernel, n_blk, half), kinds, core,
        [qkv_own] * 3 + [do_own] + [qkv_oth] * 3 + [do_oth, lse_arr],
        [part(0), part(1), part(2), one] * 2 + [lse], [three, three, sums],
        [jax.ShapeDtypeStruct((3, n_blk, half, wide), bf)] * 2 + [jax.ShapeDtypeStruct((heads, 3, 8, dim), jnp.float32)],
        [pltpu.VMEM((n_blk, blk, dim), bf)] * 4 + [pltpu.VMEM((n_blk, dim, blk), bf)]
        + [pltpu.VMEM((2, n_blk, blk, blk), jnp.float32), pltpu.VMEM((2, n_blk, blk, blk), bf)]
        + [pltpu.VMEM((n_blk, blk, dim), jnp.float32)] * 2 + [pltpu.VMEM((2, blk, dim), bf)],
        (n_blk, blk), 5)


def matmul_call(body, scalars, grid, ins, outs, out_shape, flops):
    args = [a for a, _ in ins]
    moved = sum(a.size * a.dtype.itemsize for a in args)
    return pl.pallas_call(
        body,
        grid_spec=pltpu.PrefetchScalarGridSpec(
            num_scalar_prefetch=len(scalars), grid=grid, in_specs=[spec for _, spec in ins], out_specs=outs),
        out_shape=out_shape,
        compiler_params=pltpu.CompilerParams(
            dimension_semantics=("arbitrary",) * len(grid), vmem_limit_bytes=56 * 1024 * 1024),
        cost_estimate=pl.CostEstimate(flops=flops, bytes_accessed=moved, transcendentals=0),
    )(*scalars, *args)


def project_qkv(h, w, bias, group):
    n_tok, d_model = h.shape
    wide = d_model // 2
    tile = wide // 2

    def body(g, h_ref, w_ref, b_ref, out):
        out[...] = (dot_nn(h_ref[...], w_ref[...]) + b_ref[...].astype(jnp.float32)).astype(jnp.bfloat16)

    def cols(t, j, g):
        return (0, t * 4 + g[0] * 2 + j)

    return matmul_call(
        body, [group], (3, 2),
        [(h, pl.BlockSpec((n_tok, d_model), lambda t, j, g: (0, 0))),
         (w, pl.BlockSpec((d_model, tile), cols)), (bias, pl.BlockSpec((1, tile), cols))],
        pl.BlockSpec((None, n_tok, tile), lambda t, j, g: (t, 0, j)),
        jax.ShapeDtypeStruct((3, n_tok, wide), jnp.bfloat16), 6 * n_tok * d_model * wide)


def project_do(dy, w, group):
    n_tok, d_model = dy.shape
    wide = d_model // 2
    tile = wide // 2

    def body(g, dy_ref, w_ref, out):
        out[...] = dot_nt(dy_ref[...], w_ref[...]).astype(jnp.bfloat16)

    return matmul_call(
        body, [group], (2,),
        [(dy, pl.BlockSpec((n_tok, d_model), lambda j, g: (0, 0))),
         (w, pl.BlockSpec((tile, d_model), lambda j, g: (g[0] * 2 + j, 0)))],
        pl.BlockSpec((n_tok, tile), lambda j, g: (0, j)),
        jax.ShapeDtypeStruct((n_tok, wide), jnp.bfloat16), 2 * n_tok * d_model * wide)


def out_weight_grad(o_own, o_oth, dy, core):
    n_tok, d_model = dy.shape
    wide = d_model // 2
    tile = wide // 2

    def body(c, own, oth, dy_ref, out):
        @pl.when(pl.program_id(0) == 0)
        def _():
            out[...] = dot_nn(jnp.transpose(own[...]), dy_ref[...])

        @pl.when(pl.program_id(0) == 1)
        def _():
            out[...] = dot_nn(jnp.transpose(oth[...]), dy_ref[...])

    return matmul_call(
        body, [core], (2, 2),
        [(o_own, pl.BlockSpec((n_tok, tile), lambda s, j, c: (0, j * (1 - s) + s))),
         (o_oth, pl.BlockSpec((n_tok, tile), lambda s, j, c: (0, j * s))),
         (dy, pl.BlockSpec((n_tok, d_model), lambda s, j, c: (0, 0)))],
        pl.BlockSpec((tile, d_model), lambda s, j, c: (((1 - s) * c[0] + s * (1 - c[0])) * 2 + j, 0)),
        jax.ShapeDtypeStruct((d_model, d_model), jnp.float32), 2 * n_tok * d_model * d_model)


def project_out(x, o_own, o_oth, w, bias, core):
    n_tok, d_model = x.shape
    wide = d_model // 2
    tile = d_model // 4

    def body(c, x_ref, own, oth, w_own, w_oth, b_ref, out):
        y = dot_nn(own[...], w_own[...]) + dot_nn(oth[...], w_oth[...])
        out[...] = (x_ref[...].astype(jnp.float32) + y + b_ref[...].astype(jnp.float32)).astype(jnp.bfloat16)

    whole = pl.BlockSpec((n_tok, wide), lambda j, c: (0, 0))
    return matmul_call(
        body, [core], (4,),
        [(x, pl.BlockSpec((n_tok, tile), lambda j, c: (0, j))), (o_own, whole), (o_oth, whole),
         (w, pl.BlockSpec((wide, tile), lambda j, c: (c[0], j))), (w, pl.BlockSpec((wide, tile), lambda j, c: (1 - c[0], j))),
         (bias, pl.BlockSpec((1, tile), lambda j, c: (0, j)))],
        pl.BlockSpec((n_tok, tile), lambda j, c: (0, j)),
        jax.ShapeDtypeStruct((n_tok, d_model), jnp.bfloat16), 2 * n_tok * d_model * d_model)


def hidden_grad(dg_own, dg_oth, w, core):
    _, n_tok, wide = dg_own.shape
    d_model = 2 * wide
    tile = d_model // 8

    def body(c, own, oth, *refs):
        out = refs[-1]
        total = None
        for t in range(3):
            for src, w_ref in ((own, refs[t]), (oth, refs[3 + t])):
                one = dot_nt(src[t], w_ref[...])
                total = one if total is None else total + one
        out[...] = total.astype(jnp.bfloat16)

    whole = pl.BlockSpec((3, n_tok, wide), lambda j, c: (0, 0, 0))

    def col(t, mine):
        return pl.BlockSpec((tile, wide), lambda j, c: (j, 2 * t + (c[0] if mine else 1 - c[0])))

    return matmul_call(
        body, [core], (8,),
        [(dg_own, whole), (dg_oth, whole)] + [(w, col(t, True)) for t in range(3)] + [(w, col(t, False)) for t in range(3)],
        pl.BlockSpec((n_tok, tile), lambda j, c: (0, j)),
        jax.ShapeDtypeStruct((n_tok, d_model), jnp.bfloat16), 12 * n_tok * wide * d_model)


def qkv_weight_grad(h_own, h_oth, dg_own, dg_oth):
    n_tok, d_model = h_own.shape
    wide = d_model // 2
    tile = d_model // 4

    def body(ha, hb, da, db, out):
        out[...] = dot_nn(jnp.transpose(ha[...]), da[...]) + dot_nn(jnp.transpose(hb[...]), db[...])

    h_spec = pl.BlockSpec((n_tok, tile), lambda t, i: (0, i))
    d_spec = pl.BlockSpec((None, n_tok, wide), lambda t, i: (t, 0, 0))
    return matmul_call(
        body, [], (3, 4),
        [(h_own, h_spec), (h_oth, h_spec), (dg_own, d_spec), (dg_oth, d_spec)],
        pl.BlockSpec((None, tile, wide), lambda t, i: (t, i, 0)),
        jax.ShapeDtypeStruct((3, d_model, wide), jnp.float32), 12 * n_tok * d_model * wide)


def copy_kernel(*refs):
    refs[-1][...] = refs[-2][...]


def place(piece, total_rows, first_row, dst=None):
    rows, cols = piece.shape
    tile = 128 if cols > 4096 else 512
    skip = first_row // tile
    in_specs = [pl.BlockSpec((tile, cols), lambda r: (r, 0))]
    args = [piece]
    aliases = {}
    if dst is not None:
        in_specs = [pl.BlockSpec(memory_space=pl.ANY)] + in_specs
        args = [dst] + args
        aliases = {0: 0}
    return pl.pallas_call(
        copy_kernel,
        grid=(rows // tile,),
        in_specs=in_specs,
        out_specs=pl.BlockSpec((tile, cols), lambda r: (r + skip, 0)),
        out_shape=jax.ShapeDtypeStruct((total_rows, cols), piece.dtype),
        input_output_aliases=aliases,
        cost_estimate=pl.CostEstimate(flops=rows * cols * 8, bytes_accessed=2 * piece.nbytes, transcendentals=0),
        name="place_rows",
    )(*args)


def grad_sum_kernel(n_chip, rows, g_all, small, out, small_out, acc, rc, rb, ra, slots, load_sem, loc_sem,
                    c_send, c_recv, b_send, b_recv, a_send, a_recv, g_send, g_recv, s_send, s_recv, v_send, v_recv):
    chip = lax.axis_index("chip")
    core = lax.axis_index("core")
    n_dev = 2 * n_chip
    me = chip * 2 + core
    bits = [chip % 2, (chip // 2) % 2, chip // 4]
    beside = [chip + (1 - 2 * bits[d]) * (1 << d) for d in range(3)]
    parts = [g_all.at[t] for t in range(3)]
    chunk = rows // 8
    wide = acc.shape[2]
    mesh_id = pl.DeviceIdType.MESH

    barrier = pltpu.get_barrier_semaphore()
    for o in range(1, n_dev):
        to = (me + o) % n_dev
        pl.semaphore_signal(barrier, inc=1, device_id=(to // 2, to % 2), device_id_type=mesh_id)
    pl.semaphore_wait(barrier, n_dev - 1)

    def flip(b, f):
        return 1 - b if f else b

    def remote(src, dst, send, recv, to_chip, to_core):
        c = pltpu.make_async_remote_copy(src_ref=src, dst_ref=dst, send_sem=send, recv_sem=recv,
                                         device_id=(to_chip, to_core), device_id_type=mesh_id)
        c.start()
        return c

    bc = [bits[t % 3] for t in range(3)]
    bb = [bits[(t + 1) % 3] for t in range(3)]
    ba = [bits[(t + 2) % 3] for t in range(3)]
    to_c = [beside[t % 3] for t in range(3)]
    to_b = [beside[(t + 1) % 3] for t in range(3)]
    to_a = [beside[(t + 2) % 3] for t in range(3)]

    def near(t, fb, fa):
        return pl.multiple_of(flip(bb[t], fb) * (2 * chunk) + flip(ba[t], fa) * chunk, chunk)

    def full(t, fc, fb, fa):
        return pl.multiple_of(flip(bc[t], fc) * (4 * chunk) + flip(bb[t], fb) * (2 * chunk) + flip(ba[t], fa) * chunk, chunk)

    flips = ((1, 1), (1, 0), (0, 1), (0, 0))
    c_copy = {}
    for j, (fb, fa) in enumerate(flips):
        for t in range(3):
            c_copy[t, j] = remote(parts[t].at[pl.ds(full(t, 1, fb, fa), chunk), :], rc.at[t, j],
                                  c_send.at[t, j], c_recv.at[t, j], to_c[t], core)
    loads = []
    for t in range(3):
        half_row = pl.multiple_of(bc[t] * (4 * chunk), 4 * chunk)
        load = pltpu.make_async_copy(parts[t].at[pl.ds(half_row, 4 * chunk), :], acc.at[t], load_sem.at[t])
        load.start()
        loads.append(load)
    v_copy = []
    for o in range(1, n_dev):
        to = (me + o) % n_dev
        v_copy.append(remote(small, slots.at[o], v_send.at[o], v_recv.at[o], to // 2, to % 2))
    slots[0] = small[...]
    for load in loads:
        load.wait()

    tile = 64

    def add(t, fb, fa, got):
        first = near(t, fb, fa)

        def step(i, carry):
            at = pl.ds(pl.multiple_of(first + i * tile, tile), tile)
            acc[t, at, :] = acc[t, at, :] + got[pl.ds(pl.multiple_of(i * tile, tile), tile), :]
            return carry

        lax.fori_loop(0, chunk // tile, step, 0)

    def held(t, fb, fa):
        return acc.at[t, pl.ds(near(t, fb, fa), chunk), :]

    b_copy = {}
    for j in range(2):
        fb, fa = flips[j]
        for t in range(3):
            c_copy[t, j].wait_recv()
            add(t, fb, fa, rc.at[t, j])
        for t in range(3):
            b_copy[t, j] = remote(held(t, fb, fa), rb.at[t, j], b_send.at[t, j], b_recv.at[t, j], to_b[t], core)
    for j in range(2, 4):
        fb, fa = flips[j]
        for t in range(3):
            c_copy[t, j].wait_recv()
            add(t, fb, fa, rc.at[t, j])
    a_copy = {}
    for t in range(3):
        b_copy[t, 0].wait_recv()
        add(t, 0, 1, rb.at[t, 0])
    for t in range(3):
        a_copy[t] = remote(held(t, 0, 1), ra.at[t], a_send.at[t], a_recv.at[t], to_a[t], core)
    for t in range(3):
        b_copy[t, 1].wait_recv()
        add(t, 0, 0, rb.at[t, 1])
    for t in range(3):
        a_copy[t].wait_recv()
        add(t, 0, 0, ra.at[t])

    def place_at(t, fc, fb, fa):
        return out.at[pl.ds(full(t, fc, fb, fa), chunk), pl.ds(pl.multiple_of((2 * t + core) * wide, wide), wide)]

    g_copy, s_copy, stores = {}, {}, []

    def gather(t, idx, src, dst, to):
        g_copy[t, idx] = remote(src, dst, g_send.at[t, idx], g_recv.at[t, idx], to, core)

    def share(t, idx, src, dst):
        s_copy[t, idx] = remote(src, dst, s_send.at[t, idx], s_recv.at[t, idx], chip, 1 - core)

    for idx, to in ((0, to_a), (1, to_b), (3, to_c)):
        for t in range(3):
            gather(t, idx, held(t, 0, 0), place_at(t, 0, 0, 0), to[t])
    for t in range(3):
        share(t, 0, held(t, 0, 0), place_at(t, 0, 0, 0))
        store = pltpu.make_async_copy(held(t, 0, 0), place_at(t, 0, 0, 0), loc_sem.at[t])
        store.start()
        stores.append(store)
    got_flips = ((0, 0, 1), (0, 1, 0), (0, 1, 1), (1, 0, 0), (1, 0, 1), (1, 1, 0), (1, 1, 1))
    onward = {0: ((2, to_b), (4, to_c)), 1: ((5, to_c),), 2: ((6, to_c),)}
    for idx in (0, 1, 3, 2, 4, 5, 6):
        for t in range(3):
            g_copy[t, idx].wait_recv()
            where = place_at(t, *got_flips[idx])
            for nxt, to in onward.get(idx, ()):
                gather(t, nxt, where, where, to[t])
            share(t, idx + 1, where, where)

    for copy in v_copy:
        copy.wait_recv()
    total = slots[me % n_dev]
    for d in range(1, n_dev):
        total = total + slots[(me + n_dev - d) % n_dev]
    small_out[...] = total

    for group in (s_copy,):
        for copy in group.values():
            copy.wait_recv()
    for group in (c_copy, b_copy, a_copy, g_copy, s_copy):
        for copy in group.values():
            copy.wait_send()
    for copy in v_copy:
        copy.wait_send()
    for store in stores:
        store.wait()


def grad_sum(n_chip, g_all, small):
    _, rows, wide = g_all.shape
    chunk = rows // 8
    n_dev = 2 * n_chip
    f32 = jnp.float32
    dma = pltpu.SemaphoreType.DMA
    hbm = pl.BlockSpec(memory_space=pl.ANY)
    vmem = pl.BlockSpec(memory_space=pltpu.VMEM)
    return pl.pallas_call(
        functools.partial(grad_sum_kernel, n_chip, rows),
        in_specs=[hbm, vmem],
        out_specs=[hbm, vmem],
        out_shape=[jax.ShapeDtypeStruct((rows, 6 * wide), f32), jax.ShapeDtypeStruct(small.shape, f32)],
        scratch_shapes=[
            pltpu.VMEM((3, 4 * chunk, wide), f32), pltpu.VMEM((3, 4, chunk, wide), f32),
            pltpu.VMEM((3, 2, chunk, wide), f32), pltpu.VMEM((3, chunk, wide), f32),
            pltpu.VMEM((n_dev,) + small.shape, f32), dma((3,)), dma((3,)),
            dma((3, 4)), dma((3, 4)), dma((3, 2)), dma((3, 2)), dma((3,)), dma((3,)),
            dma((3, 7)), dma((3, 7)), dma((3, 8)), dma((3, 8)), dma((n_dev,)), dma((n_dev,)),
        ],
        compiler_params=pltpu.CompilerParams(collective_id=0, has_side_effects=True, vmem_limit_bytes=44 * 1024 * 1024),
        cost_estimate=pl.CostEstimate(flops=3 * 10**11, bytes_accessed=150 * 2**20, transcendentals=0),
        name="grad_sum",
    )(g_all, small)


def solution(mesh):
    n_dev = mesh.shape["sp"]
    n_chip = n_dev // 2
    grid_mesh = Mesh(mesh.devices.reshape(n_chip, 2), ("chip", "core"))
    tok_spec = P(None, ("chip", "core"), None)
    swap_pairs = [(0, 1), (1, 0)]

    def local_block(x, d_y, ln_gamma, ln_beta, w_qkv, b_qkv, w_out, b_out, head_kind):
        half = x.shape[1]
        d_model = x.shape[2]
        num_heads = head_kind.shape[0]
        own_heads = num_heads // 2
        wide = d_model // 2
        n_tok = n_chip * half
        f32, bf = jnp.float32, jnp.bfloat16
        core = lax.axis_index("core")
        core_arr = jnp.full((1,), core, jnp.int32)
        my_kinds = lax.dynamic_slice_in_dim(head_kind, core * own_heads, own_heads)

        def swap(v):
            return lax.ppermute(v, "core", swap_pairs)

        x_b = lax.all_to_all(x, "chip", 0, 0, tiled=True).reshape(n_tok, d_model)
        g_b = lax.all_to_all(d_y, "chip", 0, 0, tiled=True).reshape(n_tok, d_model)

        other_arr = 1 - core_arr
        blocks = (3, n_chip, half, wide)

        x_f = x_b.astype(f32)
        h_f, ln_pull = jax.vjp(layer_norm, x_f, ln_gamma.astype(f32), ln_beta.astype(f32))
        h_norm = h_f.astype(bf)
        bias_row = b_qkv.reshape(1, 3 * d_model)
        qkv_send = project_qkv(h_norm, w_qkv, bias_row, other_arr)
        qkv_oth = swap(qkv_send).reshape(blocks)
        qkv_own = project_qkv(h_norm, w_qkv, bias_row, core_arr).reshape(blocks)
        g_b, qkv_own = lax.optimization_barrier((g_b, qkv_own))
        o_own, o_send, lse = attention_forward(my_kinds, core_arr, qkv_own, qkv_oth)
        o_oth = swap(o_send).reshape(n_tok, wide)
        o_own = o_own.reshape(n_tok, wide)
        do_oth = swap(project_do(g_b, w_out, other_arr)).reshape(blocks[1:])
        do_own = project_do(g_b, w_out, core_arr).reshape(blocks[1:])
        h_oth = swap(h_norm)

        d_wout = out_weight_grad(o_own, o_oth, g_b, core_arr)
        y_b = project_out(x_b, o_own, o_oth, w_out, b_out.reshape(1, d_model), core_arr)
        y_b, do_own, do_oth = lax.optimization_barrier((y_b, do_own, do_oth))
        d_wout = lax.psum(d_wout, ("chip", "core"))
        y_out = lax.all_to_all(y_b.reshape(n_chip, half, d_model), "chip", 0, 0, tiled=True)

        dg_own, dg_send, bias_sums = attention_backward(my_kinds, core_arr, qkv_own, do_own, qkv_oth, do_oth, lse)
        dg_oth = swap(dg_send).reshape(3, n_tok, wide)
        dg_own = dg_own.reshape(3, n_tok, wide)
        dg_send = dg_send.reshape(3, n_tok, wide)

        d_h = hidden_grad(dg_own, dg_oth, w_qkv, core_arr).astype(f32)
        d_x_ln, d_gamma, d_beta = ln_pull(d_h)
        d_x_b = (g_b.astype(f32) + d_x_ln).astype(bf)
        d_x = lax.all_to_all(d_x_b.reshape(n_chip, half, d_model), "chip", 0, 0, tiled=True)
        bias_mine = jnp.sum(bias_sums, axis=2).transpose(1, 0, 2).reshape(3, 1, wide)
        d_bqkv = jnp.where(lax.broadcasted_iota(jnp.int32, (3, 2, wide), 1) == core, bias_mine, 0.0).reshape(3 * d_model)
        d_bout = jnp.sum(g_b, axis=0, dtype=f32)

        d_w = qkv_weight_grad(h_norm, h_oth, dg_own, dg_send)
        small = jnp.concatenate([d_gamma, d_beta, d_bqkv, d_bout]).reshape(-1, 128)
        d_wqkv, small = grad_sum(n_chip, d_w, small)
        d_wqkv = place(d_wqkv, d_model, 0)
        small = small.reshape(-1)
        d_gamma, d_beta, d_bqkv, d_bout = (small[:d_model], small[d_model:2 * d_model], small[2 * d_model:5 * d_model], small[5 * d_model:])
        d_wout = place(d_wout, d_model, 0)
        y_out = place(y_out.reshape(n_tok, d_model), n_tok, 0).reshape(n_chip, half, d_model)
        d_x = place(d_x.reshape(n_tok, d_model), n_tok, 0).reshape(n_chip, half, d_model)
        return y_out, d_x, d_gamma, d_beta, d_wqkv, d_bqkv, d_wout, d_bout

    return jax.shard_map(
        local_block, mesh=grid_mesh,
        in_specs=(tok_spec, tok_spec, P(), P(), P(), P(), P(), P(), P()),
        out_specs=(tok_spec, tok_spec, P(), P(), P(), P(), P(), P()), check_vma=False)
```

```python
import functools
import math
import jax
import jax.numpy as jnp
from jax import lax
from jax.experimental import pallas as pl
from jax.experimental.pallas import tpu as pltpu
from jax.sharding import Mesh, PartitionSpec as P

LN_EPS = 1e-5
NEG_BIG = -1e30
LOG2_E = 1.4426950408889634


def layer_norm(x_rows, gamma_f, beta_f):
    row_mean = jnp.mean(x_rows, axis=-1, keepdims=True)
    centred = x_rows - row_mean
    row_var = jnp.mean(centred * centred, axis=-1, keepdims=True)
    return centred * lax.rsqrt(row_var + LN_EPS) * gamma_f + beta_f


def dot_nn(a, b):
    return lax.dot_general(a, b, (((1,), (0,)), ((), ())), preferred_element_type=jnp.float32)


def dot_nt(a, b):
    return lax.dot_general(a, b, (((1,), (1,)), ((), ())), preferred_element_type=jnp.float32)


def fold(x, op):
    return op(x.reshape(x.shape[0] // 8, 8, x.shape[1]), axis=0)


def merge_halves(n_blk, half, at_a, at_b, triples):
    for dst, src_a, src_b in triples:
        for c in range(n_blk):
            dst[c, pl.ds(at_a, half), :] = src_a[c]
            dst[c, pl.ds(at_b, half), :] = src_b[c]


def block_cases(group, banded, process):
    for i in range(2):
        @pl.when((group == i) & jnp.logical_not(banded))
        def _():
            process(list(range(4 * i + 4)), [(0, 4 * i + r + 1, False) for r in range(4)])

    @pl.when((group == 0) & banded)
    def _():
        process(list(range(4)), [(0, 1, False), (0, 2, False), (0, 3, True), (1, 4, True)])

    @pl.when((group == 1) & banded)
    def _():
        process(list(range(2, 8)), [(r, r + 3, True) for r in range(4)])


def masked_scores(k, q, factor, last, band_first):
    s = dot_nt(k, q) * factor
    if last or band_first:
        row = lax.broadcasted_iota(jnp.int32, s.shape, 0)
        col = lax.broadcasted_iota(jnp.int32, s.shape, 1)
        s = jnp.where(row <= col if last else row > col, s, NEG_BIG)
    return s


def plus(total, part):
    return part if total is None else total + part


def forward_kernel(n_blk, half, kind_ref, core_ref, qa, ka, va, qb, kb, vb, oa, ob, lse, qs, ks, vs, vt, s_scr, out_scr):
    group = pl.program_id(1)
    core = core_ref[0]
    factor = LOG2_E / math.sqrt(qs.shape[2])
    at_a = pl.multiple_of(core * half, half)
    at_b = pl.multiple_of((1 - core) * half, half)

    @pl.when(group == 0)
    def _():
        merge_halves(n_blk, half, at_a, at_b, ((qs, qa, qb), (ks, ka, kb), (vs, va, vb)))
        for c in range(n_blk):
            vt[c] = jnp.transpose(vs[c])

    def process(chunks, ranges):
        tops, sums = [None] * 4, [None] * 4
        for idx, c in enumerate(chunks):
            for r, (lo, hi, edge) in enumerate(ranges):
                if lo <= idx < hi:
                    s = masked_scores(ks[c], qs[4 * group + r], factor, idx == hi - 1, edge and idx == lo)
                    s_scr[r, idx] = s
                    part = fold(s, jnp.max)
                    tops[r] = part if tops[r] is None else jnp.maximum(tops[r], part)
        for r, (lo, hi, edge) in enumerate(ranges):
            tops[r] = jnp.max(tops[r], axis=0, keepdims=True)
            for idx in range(lo, hi):
                e = jnp.exp2(s_scr[r, idx] - tops[r])
                s_scr[r, idx] = e
                sums[r] = plus(sums[r], fold(e, jnp.sum))
        for r, (lo, hi, edge) in enumerate(ranges):
            total = jnp.sum(sums[r], axis=0, keepdims=True)
            inv = 1.0 / total
            o_t = None
            for idx in range(lo, hi):
                o_t = plus(o_t, dot_nn(vt[chunks[idx]], (s_scr[r, idx] * inv).astype(jnp.bfloat16)))
            out_scr[r] = jnp.transpose(o_t).astype(jnp.bfloat16)
            lse[4 * group + r] = jnp.broadcast_to(tops[r] + jnp.log2(total), lse.shape[1:])

    block_cases(group, kind_ref[pl.program_id(0)] == 1, process)
    for r in range(4):
        oa[4 * group + r] = out_scr[r, pl.ds(at_a, half), :]
        ob[4 * group + r] = out_scr[r, pl.ds(at_b, half), :]


def backward_kernel(n_blk, half, kind_ref, core_ref, qa, ka, va, ga, qb, kb, vb, gb, lse, da, db, bias,
                    qs, ks, vs, gs, kt, p_scr, dp_scr, dk_scr, dv_scr, out_scr):
    group = pl.program_id(1)
    core = core_ref[0]
    scale = 1.0 / math.sqrt(qs.shape[2])
    at_a = pl.multiple_of(core * half, half)
    at_b = pl.multiple_of((1 - core) * half, half)

    @pl.when(group == 0)
    def _():
        merge_halves(n_blk, half, at_a, at_b, ((qs, qa, qb), (ks, ka, kb), (vs, va, vb), (gs, ga, gb)))
        for c in range(n_blk):
            kt[c] = jnp.transpose(ks[c])
        dk_scr[...] = jnp.zeros_like(dk_scr)
        dv_scr[...] = jnp.zeros_like(dv_scr)
        bias[...] = jnp.zeros_like(bias)

    def process(chunks, ranges):
        deltas, dq_t = [None] * 4, [None] * 4
        for idx, c in enumerate(chunks):
            dv = None
            for r, (lo, hi, edge) in enumerate(ranges):
                if lo <= idx < hi:
                    qi = 4 * group + r
                    s = masked_scores(ks[c], qs[qi], scale * LOG2_E, idx == hi - 1, edge and idx == lo)
                    p = jnp.exp2(s - lse[qi][0:1])
                    p_scr[r, idx] = p
                    dp = dot_nt(vs[c], gs[qi]).astype(jnp.bfloat16)
                    dp_scr[r, idx] = dp
                    deltas[r] = plus(deltas[r], fold(p * dp.astype(jnp.float32), jnp.sum))
                    dv = plus(dv, dot_nn(p.astype(jnp.bfloat16), gs[qi]))
            dv_scr[c] += dv
        deltas = [jnp.sum(d, axis=0, keepdims=True) for d in deltas]
        for idx, c in enumerate(chunks):
            dk = None
            for r, (lo, hi, edge) in enumerate(ranges):
                if lo <= idx < hi:
                    ds = (p_scr[r, idx] * (dp_scr[r, idx].astype(jnp.float32) - deltas[r])).astype(jnp.bfloat16)
                    dq_t[r] = plus(dq_t[r], dot_nn(kt[c], ds))
                    dk = plus(dk, dot_nn(ds, qs[4 * group + r]))
            dk_scr[c] += dk
        for r in range(4):
            out_scr[r] = jnp.transpose(dq_t[r] * scale).astype(jnp.bfloat16)

    block_cases(group, kind_ref[pl.program_id(0)] == 1, process)

    def give(part, c, slot):
        bias[part] += fold(out_scr[slot].astype(jnp.float32), jnp.sum)
        da[part, c] = out_scr[slot, pl.ds(at_a, half), :]
        db[part, c] = out_scr[slot, pl.ds(at_b, half), :]

    for r in range(4):
        give(0, 4 * group + r, r)

    @pl.when(group == 1)
    def _():
        for c in range(n_blk):
            out_scr[0] = (dk_scr[c] * scale).astype(jnp.bfloat16)
            out_scr[1] = dv_scr[c].astype(jnp.bfloat16)
            give(1, c, 0)
            give(2, c, 1)


def head_specs(n_blk, half, dim):
    def part(t):
        return pl.BlockSpec((None, n_blk, half, dim), lambda h, i, kind, cr: (t, 0, 0, h))

    one = pl.BlockSpec((n_blk, half, dim), lambda h, i, kind, cr: (0, 0, h))
    three = pl.BlockSpec((3, n_blk, half, dim), lambda h, i, kind, cr: (0, 0, 0, h))
    lse = pl.BlockSpec((None, n_blk, 8, 2 * half), lambda h, i, kind, cr: (h, 0, 0, 0))
    sums = pl.BlockSpec((None, 3, 8, dim), lambda h, i, kind, cr: (h, 0, 0, 0))
    return part, one, three, lse, sums


def attention_call(body, kinds, core, args, in_specs, out_specs, out_shape, scratch, n_tok, products):
    heads = kinds.shape[0]
    return pl.pallas_call(
        body,
        grid_spec=pltpu.PrefetchScalarGridSpec(
            num_scalar_prefetch=2, grid=(heads, 2), in_specs=in_specs, out_specs=out_specs, scratch_shapes=scratch),
        out_shape=out_shape,
        compiler_params=pltpu.CompilerParams(
            dimension_semantics=("arbitrary", "arbitrary"), vmem_limit_bytes=48 * 1024 * 1024),
        cost_estimate=pl.CostEstimate(
            flops=products * heads * (n_tok[0] * n_tok[1]) ** 2 * 128, bytes_accessed=24 * 2**20,
            transcendentals=heads * (n_tok[0] * n_tok[1]) ** 2 // 2),
    )(kinds, core, *args)


def attention_forward(kinds, core, qkv_own, qkv_oth):
    _, n_blk, half, wide = qkv_own.shape
    heads = kinds.shape[0]
    dim = wide // heads
    blk = 2 * half
    bf = jnp.bfloat16
    part, one, _, lse, _ = head_specs(n_blk, half, dim)
    return attention_call(
        functools.partial(forward_kernel, n_blk, half), kinds, core, [qkv_own] * 3 + [qkv_oth] * 3,
        [part(0), part(1), part(2)] * 2, [one, one, lse],
        [jax.ShapeDtypeStruct((n_blk, half, wide), bf)] * 2 + [jax.ShapeDtypeStruct((heads, n_blk, 8, blk), jnp.float32)],
        [pltpu.VMEM((n_blk, blk, dim), bf)] * 3 + [pltpu.VMEM((n_blk, dim, blk), bf)]
        + [pltpu.VMEM((4, n_blk, blk, blk), jnp.float32), pltpu.VMEM((4, blk, dim), bf)],
        (n_blk, blk), 2)


def attention_backward(kinds, core, qkv_own, do_own, qkv_oth, do_oth, lse_arr):
    _, n_blk, half, wide = qkv_own.shape
    heads = kinds.shape[0]
    dim = wide // heads
    blk = 2 * half
    bf = jnp.bfloat16
    part, one, three, lse, sums = head_specs(n_blk, half, dim)
    return attention_call(
        functools.partial(backward_kernel, n_blk, half), kinds, core,
        [qkv_own] * 3 + [do_own] + [qkv_oth] * 3 + [do_oth, lse_arr],
        [part(0), part(1), part(2), one] * 2 + [lse], [three, three, sums],
        [jax.ShapeDtypeStruct((3, n_blk, half, wide), bf)] * 2 + [jax.ShapeDtypeStruct((heads, 3, 8, dim), jnp.float32)],
        [pltpu.VMEM((n_blk, blk, dim), bf)] * 4 + [pltpu.VMEM((n_blk, dim, blk), bf)]
        + [pltpu.VMEM((4, n_blk, blk, blk), jnp.float32), pltpu.VMEM((4, n_blk, blk, blk), bf)]
        + [pltpu.VMEM((n_blk, blk, dim), jnp.float32)] * 2 + [pltpu.VMEM((4, blk, dim), bf)],
        (n_blk, blk), 5)


def matmul_call(body, scalars, grid, ins, outs, out_shape, flops):
    args = [a for a, _ in ins]
    moved = sum(a.size * a.dtype.itemsize for a in args)
    return pl.pallas_call(
        body,
        grid_spec=pltpu.PrefetchScalarGridSpec(
            num_scalar_prefetch=len(scalars), grid=grid, in_specs=[spec for _, spec in ins], out_specs=outs),
        out_shape=out_shape,
        compiler_params=pltpu.CompilerParams(
            dimension_semantics=("arbitrary",) * len(grid), vmem_limit_bytes=56 * 1024 * 1024),
        cost_estimate=pl.CostEstimate(flops=flops, bytes_accessed=moved, transcendentals=0),
    )(*scalars, *args)


def project_qkv(h, w, bias, group):
    n_tok, d_model = h.shape
    wide = d_model // 2
    tile = wide // 2

    def body(g, h_ref, w_ref, b_ref, out):
        out[...] = (dot_nn(h_ref[...], w_ref[...]) + b_ref[...].astype(jnp.float32)).astype(jnp.bfloat16)

    def cols(t, j, g):
        return (0, t * 4 + g[0] * 2 + j)

    return matmul_call(
        body, [group], (3, 2),
        [(h, pl.BlockSpec((n_tok, d_model), lambda t, j, g: (0, 0))),
         (w, pl.BlockSpec((d_model, tile), cols)), (bias, pl.BlockSpec((1, tile), cols))],
        pl.BlockSpec((None, n_tok, tile), lambda t, j, g: (t, 0, j)),
        jax.ShapeDtypeStruct((3, n_tok, wide), jnp.bfloat16), 6 * n_tok * d_model * wide)


def project_do(dy, w, group):
    n_tok, d_model = dy.shape
    wide = d_model // 2
    tile = wide // 2

    def body(g, dy_ref, w_ref, out):
        out[...] = dot_nt(dy_ref[...], w_ref[...]).astype(jnp.bfloat16)

    return matmul_call(
        body, [group], (2,),
        [(dy, pl.BlockSpec((n_tok, d_model), lambda j, g: (0, 0))),
         (w, pl.BlockSpec((tile, d_model), lambda j, g: (g[0] * 2 + j, 0)))],
        pl.BlockSpec((n_tok, tile), lambda j, g: (0, j)),
        jax.ShapeDtypeStruct((n_tok, wide), jnp.bfloat16), 2 * n_tok * d_model * wide)


def out_weight_grad(o_own, o_oth, dy, core):
    n_tok, d_model = dy.shape
    wide = d_model // 2
    tile = wide // 2

    def body(c, own, oth, dy_ref, out):
        @pl.when(pl.program_id(0) == 0)
        def _():
            out[...] = dot_nn(jnp.transpose(own[...]), dy_ref[...])

        @pl.when(pl.program_id(0) == 1)
        def _():
            out[...] = dot_nn(jnp.transpose(oth[...]), dy_ref[...])

    return matmul_call(
        body, [core], (2, 2),
        [(o_own, pl.BlockSpec((n_tok, tile), lambda s, j, c: (0, j * (1 - s) + s))),
         (o_oth, pl.BlockSpec((n_tok, tile), lambda s, j, c: (0, j * s))),
         (dy, pl.BlockSpec((n_tok, d_model), lambda s, j, c: (0, 0)))],
        pl.BlockSpec((tile, d_model), lambda s, j, c: (((1 - s) * c[0] + s * (1 - c[0])) * 2 + j, 0)),
        jax.ShapeDtypeStruct((d_model, d_model), jnp.float32), 2 * n_tok * d_model * d_model)


def project_out(x, o_own, o_oth, w, bias, core):
    n_tok, d_model = x.shape
    wide = d_model // 2
    tile = d_model // 4

    def body(c, x_ref, own, oth, w_own, w_oth, b_ref, out):
        y = dot_nn(own[...], w_own[...]) + dot_nn(oth[...], w_oth[...])
        out[...] = (x_ref[...].astype(jnp.float32) + y + b_ref[...].astype(jnp.float32)).astype(jnp.bfloat16)

    whole = pl.BlockSpec((n_tok, wide), lambda j, c: (0, 0))
    return matmul_call(
        body, [core], (4,),
        [(x, pl.BlockSpec((n_tok, tile), lambda j, c: (0, j))), (o_own, whole), (o_oth, whole),
         (w, pl.BlockSpec((wide, tile), lambda j, c: (c[0], j))), (w, pl.BlockSpec((wide, tile), lambda j, c: (1 - c[0], j))),
         (bias, pl.BlockSpec((1, tile), lambda j, c: (0, j)))],
        pl.BlockSpec((n_tok, tile), lambda j, c: (0, j)),
        jax.ShapeDtypeStruct((n_tok, d_model), jnp.bfloat16), 2 * n_tok * d_model * d_model)


def hidden_grad(dg_own, dg_oth, w, core):
    _, n_tok, wide = dg_own.shape
    d_model = 2 * wide
    tile = d_model // 8

    def body(c, own, oth, *refs):
        out = refs[-1]
        total = None
        for t in range(3):
            for src, w_ref in ((own, refs[t]), (oth, refs[3 + t])):
                one = dot_nt(src[t], w_ref[...])
                total = one if total is None else total + one
        out[...] = total.astype(jnp.bfloat16)

    whole = pl.BlockSpec((3, n_tok, wide), lambda j, c: (0, 0, 0))

    def col(t, mine):
        return pl.BlockSpec((tile, wide), lambda j, c: (j, 2 * t + (c[0] if mine else 1 - c[0])))

    return matmul_call(
        body, [core], (8,),
        [(dg_own, whole), (dg_oth, whole)] + [(w, col(t, True)) for t in range(3)] + [(w, col(t, False)) for t in range(3)],
        pl.BlockSpec((n_tok, tile), lambda j, c: (0, j)),
        jax.ShapeDtypeStruct((n_tok, d_model), jnp.bfloat16), 12 * n_tok * wide * d_model)


def qkv_weight_grad(h_own, h_oth, dg_own, dg_oth):
    n_tok, d_model = h_own.shape
    wide = d_model // 2
    tile = d_model // 4

    def body(ha, hb, da, db, out):
        out[...] = dot_nn(jnp.transpose(ha[...]), da[...]) + dot_nn(jnp.transpose(hb[...]), db[...])

    h_spec = pl.BlockSpec((n_tok, tile), lambda t, i: (0, i))
    d_spec = pl.BlockSpec((None, n_tok, wide), lambda t, i: (t, 0, 0))
    return matmul_call(
        body, [], (3, 4),
        [(h_own, h_spec), (h_oth, h_spec), (dg_own, d_spec), (dg_oth, d_spec)],
        pl.BlockSpec((None, tile, wide), lambda t, i: (t, i, 0)),
        jax.ShapeDtypeStruct((3, d_model, wide), jnp.float32), 12 * n_tok * d_model * wide)


def copy_kernel(*refs):
    refs[-1][...] = refs[-2][...]


def place(piece, total_rows, first_row, dst=None):
    rows, cols = piece.shape
    tile = 128 if cols > 4096 else 512
    skip = first_row // tile
    in_specs = [pl.BlockSpec((tile, cols), lambda r: (r, 0))]
    args = [piece]
    aliases = {}
    if dst is not None:
        in_specs = [pl.BlockSpec(memory_space=pl.ANY)] + in_specs
        args = [dst] + args
        aliases = {0: 0}
    return pl.pallas_call(
        copy_kernel,
        grid=(rows // tile,),
        in_specs=in_specs,
        out_specs=pl.BlockSpec((tile, cols), lambda r: (r + skip, 0)),
        out_shape=jax.ShapeDtypeStruct((total_rows, cols), piece.dtype),
        input_output_aliases=aliases,
        cost_estimate=pl.CostEstimate(flops=rows * cols * 8, bytes_accessed=2 * piece.nbytes, transcendentals=0),
        name="place_rows",
    )(*args)


def grad_sum_kernel(n_chip, rows, g_all, small, out, small_out, acc, rc, rb, ra, slots, load_sem, loc_sem,
                    c_send, c_recv, b_send, b_recv, a_send, a_recv, g_send, g_recv, s_send, s_recv, v_send, v_recv):
    chip = lax.axis_index("chip")
    core = lax.axis_index("core")
    n_dev = 2 * n_chip
    me = chip * 2 + core
    bits = [chip % 2, (chip // 2) % 2, chip // 4]
    beside = [chip + (1 - 2 * bits[d]) * (1 << d) for d in range(3)]
    parts = [g_all.at[t] for t in range(3)]
    chunk = rows // 8
    wide = acc.shape[2]
    mesh_id = pl.DeviceIdType.MESH

    barrier = pltpu.get_barrier_semaphore()
    for o in range(1, n_dev):
        to = (me + o) % n_dev
        pl.semaphore_signal(barrier, inc=1, device_id=(to // 2, to % 2), device_id_type=mesh_id)
    pl.semaphore_wait(barrier, n_dev - 1)

    def flip(b, f):
        return 1 - b if f else b

    def remote(src, dst, send, recv, to_chip, to_core):
        c = pltpu.make_async_remote_copy(src_ref=src, dst_ref=dst, send_sem=send, recv_sem=recv,
                                         device_id=(to_chip, to_core), device_id_type=mesh_id)
        c.start()
        return c

    bc = [bits[t % 3] for t in range(3)]
    bb = [bits[(t + 1) % 3] for t in range(3)]
    ba = [bits[(t + 2) % 3] for t in range(3)]
    to_c = [beside[t % 3] for t in range(3)]
    to_b = [beside[(t + 1) % 3] for t in range(3)]
    to_a = [beside[(t + 2) % 3] for t in range(3)]

    def near(t, fb, fa):
        return pl.multiple_of(flip(bb[t], fb) * (2 * chunk) + flip(ba[t], fa) * chunk, chunk)

    def full(t, fc, fb, fa):
        return pl.multiple_of(flip(bc[t], fc) * (4 * chunk) + flip(bb[t], fb) * (2 * chunk) + flip(ba[t], fa) * chunk, chunk)

    flips = ((1, 1), (1, 0), (0, 1), (0, 0))
    c_copy = {}
    for j, (fb, fa) in enumerate(flips):
        for t in range(3):
            c_copy[t, j] = remote(parts[t].at[pl.ds(full(t, 1, fb, fa), chunk), :], rc.at[t, j],
                                  c_send.at[t, j], c_recv.at[t, j], to_c[t], core)
    loads = []
    for t in range(3):
        half_row = pl.multiple_of(bc[t] * (4 * chunk), 4 * chunk)
        load = pltpu.make_async_copy(parts[t].at[pl.ds(half_row, 4 * chunk), :], acc.at[t], load_sem.at[t])
        load.start()
        loads.append(load)
    v_copy = []
    for o in range(1, n_dev):
        to = (me + o) % n_dev
        v_copy.append(remote(small, slots.at[o], v_send.at[o], v_recv.at[o], to // 2, to % 2))
    slots[0] = small[...]
    for load in loads:
        load.wait()

    tile = 64

    def add(t, fb, fa, got):
        first = near(t, fb, fa)

        def step(i, carry):
            at = pl.ds(pl.multiple_of(first + i * tile, tile), tile)
            acc[t, at, :] = acc[t, at, :] + got[pl.ds(pl.multiple_of(i * tile, tile), tile), :]
            return carry

        lax.fori_loop(0, chunk // tile, step, 0)

    def held(t, fb, fa):
        return acc.at[t, pl.ds(near(t, fb, fa), chunk), :]

    b_copy = {}
    for j in range(2):
        fb, fa = flips[j]
        for t in range(3):
            c_copy[t, j].wait_recv()
            add(t, fb, fa, rc.at[t, j])
        for t in range(3):
            b_copy[t, j] = remote(held(t, fb, fa), rb.at[t, j], b_send.at[t, j], b_recv.at[t, j], to_b[t], core)
    for j in range(2, 4):
        fb, fa = flips[j]
        for t in range(3):
            c_copy[t, j].wait_recv()
            add(t, fb, fa, rc.at[t, j])
    a_copy = {}
    for t in range(3):
        b_copy[t, 0].wait_recv()
        add(t, 0, 1, rb.at[t, 0])
    for t in range(3):
        a_copy[t] = remote(held(t, 0, 1), ra.at[t], a_send.at[t], a_recv.at[t], to_a[t], core)
    for t in range(3):
        b_copy[t, 1].wait_recv()
        add(t, 0, 0, rb.at[t, 1])
    for t in range(3):
        a_copy[t].wait_recv()
        add(t, 0, 0, ra.at[t])

    def place_at(t, fc, fb, fa):
        return out.at[pl.ds(full(t, fc, fb, fa), chunk), pl.ds(pl.multiple_of((2 * t + core) * wide, wide), wide)]

    g_copy, s_copy, stores = {}, {}, []

    def gather(t, idx, src, dst, to):
        g_copy[t, idx] = remote(src, dst, g_send.at[t, idx], g_recv.at[t, idx], to, core)

    def share(t, idx, src, dst):
        s_copy[t, idx] = remote(src, dst, s_send.at[t, idx], s_recv.at[t, idx], chip, 1 - core)

    for idx, to in ((0, to_a), (1, to_b), (3, to_c)):
        for t in range(3):
            gather(t, idx, held(t, 0, 0), place_at(t, 0, 0, 0), to[t])
    for t in range(3):
        share(t, 0, held(t, 0, 0), place_at(t, 0, 0, 0))
        store = pltpu.make_async_copy(held(t, 0, 0), place_at(t, 0, 0, 0), loc_sem.at[t])
        store.start()
        stores.append(store)
    got_flips = ((0, 0, 1), (0, 1, 0), (0, 1, 1), (1, 0, 0), (1, 0, 1), (1, 1, 0), (1, 1, 1))
    onward = {0: ((2, to_b), (4, to_c)), 1: ((5, to_c),), 2: ((6, to_c),)}
    for idx in (0, 1, 3, 2, 4, 5, 6):
        for t in range(3):
            g_copy[t, idx].wait_recv()
            where = place_at(t, *got_flips[idx])
            for nxt, to in onward.get(idx, ()):
                gather(t, nxt, where, where, to[t])
            share(t, idx + 1, where, where)

    for copy in v_copy:
        copy.wait_recv()
    total = slots[me % n_dev]
    for d in range(1, n_dev):
        total = total + slots[(me + n_dev - d) % n_dev]
    small_out[...] = total

    for group in (s_copy,):
        for copy in group.values():
            copy.wait_recv()
    for group in (c_copy, b_copy, a_copy, g_copy, s_copy):
        for copy in group.values():
            copy.wait_send()
    for copy in v_copy:
        copy.wait_send()
    for store in stores:
        store.wait()


def grad_sum(n_chip, g_all, small):
    _, rows, wide = g_all.shape
    chunk = rows // 8
    n_dev = 2 * n_chip
    f32 = jnp.float32
    dma = pltpu.SemaphoreType.DMA
    hbm = pl.BlockSpec(memory_space=pl.ANY)
    vmem = pl.BlockSpec(memory_space=pltpu.VMEM)
    return pl.pallas_call(
        functools.partial(grad_sum_kernel, n_chip, rows),
        in_specs=[hbm, vmem],
        out_specs=[hbm, vmem],
        out_shape=[jax.ShapeDtypeStruct((rows, 6 * wide), f32), jax.ShapeDtypeStruct(small.shape, f32)],
        scratch_shapes=[
            pltpu.VMEM((3, 4 * chunk, wide), f32), pltpu.VMEM((3, 4, chunk, wide), f32),
            pltpu.VMEM((3, 2, chunk, wide), f32), pltpu.VMEM((3, chunk, wide), f32),
            pltpu.VMEM((n_dev,) + small.shape, f32), dma((3,)), dma((3,)),
            dma((3, 4)), dma((3, 4)), dma((3, 2)), dma((3, 2)), dma((3,)), dma((3,)),
            dma((3, 7)), dma((3, 7)), dma((3, 8)), dma((3, 8)), dma((n_dev,)), dma((n_dev,)),
        ],
        compiler_params=pltpu.CompilerParams(collective_id=0, has_side_effects=True, vmem_limit_bytes=44 * 1024 * 1024),
        cost_estimate=pl.CostEstimate(flops=3 * 10**11, bytes_accessed=150 * 2**20, transcendentals=0),
        name="grad_sum",
    )(g_all, small)


def solution(mesh):
    n_dev = mesh.shape["sp"]
    n_chip = n_dev // 2
    grid_mesh = Mesh(mesh.devices.reshape(n_chip, 2), ("chip", "core"))
    tok_spec = P(None, ("chip", "core"), None)
    swap_pairs = [(0, 1), (1, 0)]

    def local_block(x, d_y, ln_gamma, ln_beta, w_qkv, b_qkv, w_out, b_out, head_kind):
        half = x.shape[1]
        d_model = x.shape[2]
        num_heads = head_kind.shape[0]
        own_heads = num_heads // 2
        wide = d_model // 2
        n_tok = n_chip * half
        f32, bf = jnp.float32, jnp.bfloat16
        core = lax.axis_index("core")
        core_arr = jnp.full((1,), core, jnp.int32)
        my_kinds = lax.dynamic_slice_in_dim(head_kind, core * own_heads, own_heads)

        def swap(v):
            return lax.ppermute(v, "core", swap_pairs)

        x_b = lax.all_to_all(x, "chip", 0, 0, tiled=True).reshape(n_tok, d_model)
        g_b = lax.all_to_all(d_y, "chip", 0, 0, tiled=True).reshape(n_tok, d_model)

        other_arr = 1 - core_arr
        blocks = (3, n_chip, half, wide)

        x_f = x_b.astype(f32)
        h_f, ln_pull = jax.vjp(layer_norm, x_f, ln_gamma.astype(f32), ln_beta.astype(f32))
        h_norm = h_f.astype(bf)
        bias_row = b_qkv.reshape(1, 3 * d_model)
        qkv_send = project_qkv(h_norm, w_qkv, bias_row, other_arr)
        qkv_oth = swap(qkv_send).reshape(blocks)
        qkv_own = project_qkv(h_norm, w_qkv, bias_row, core_arr).reshape(blocks)
        g_b, qkv_own = lax.optimization_barrier((g_b, qkv_own))
        o_own, o_send, lse = attention_forward(my_kinds, core_arr, qkv_own, qkv_oth)
        o_oth = swap(o_send).reshape(n_tok, wide)
        o_own = o_own.reshape(n_tok, wide)
        do_send = project_do(g_b, w_out, other_arr)
        do_oth = swap(do_send).reshape(blocks[1:])
        do_own = project_do(g_b, w_out, core_arr).reshape(blocks[1:])
        h_oth = swap(h_norm)

        d_wout = out_weight_grad(o_own, o_oth, g_b, core_arr)
        y_b = project_out(x_b, o_own, o_oth, w_out, b_out.reshape(1, d_model), core_arr)
        y_b, do_own, do_oth = lax.optimization_barrier((y_b, do_own, do_oth))
        d_wout = lax.psum(d_wout, ("chip", "core"))
        y_out = lax.all_to_all(y_b.reshape(n_chip, half, d_model), "chip", 0, 0, tiled=True)

        dg_own, dg_send, bias_sums = attention_backward(my_kinds, core_arr, qkv_own, do_own, qkv_oth, do_oth, lse)
        dg_oth = swap(dg_send).reshape(3, n_tok, wide)
        dg_own = dg_own.reshape(3, n_tok, wide)
        dg_send = dg_send.reshape(3, n_tok, wide)

        d_h = hidden_grad(dg_own, dg_oth, w_qkv, core_arr).astype(f32)
        d_x_ln, d_gamma, d_beta = ln_pull(d_h)
        d_x_b = (g_b.astype(f32) + d_x_ln).astype(bf)
        d_x = lax.all_to_all(d_x_b.reshape(n_chip, half, d_model), "chip", 0, 0, tiled=True)
        bias_mine = jnp.sum(bias_sums, axis=2).transpose(1, 0, 2).reshape(3, 1, wide)
        d_bqkv = jnp.where(lax.broadcasted_iota(jnp.int32, (3, 2, wide), 1) == core, bias_mine, 0.0).reshape(3 * d_model)
        d_bout = jnp.sum(g_b, axis=0, dtype=f32)

        d_w = qkv_weight_grad(h_norm, h_oth, dg_own, dg_send)
        small = jnp.concatenate([d_gamma, d_beta, d_bqkv, d_bout]).reshape(-1, 128)
        d_wqkv, small = grad_sum(n_chip, d_w, small)
        d_wqkv = place(d_wqkv, d_model, 0)
        small = small.reshape(-1)
        d_gamma, d_beta, d_bqkv, d_bout = (small[:d_model], small[d_model:2 * d_model], small[2 * d_model:5 * d_model], small[5 * d_model:])
        d_wout = place(d_wout, d_model, 0)
        y_out = place(y_out.reshape(n_tok, d_model), n_tok, 0).reshape(n_chip, half, d_model)
        d_x = place(d_x.reshape(n_tok, d_model), n_tok, 0).reshape(n_chip, half, d_model)
        return y_out, d_x, d_gamma, d_beta, d_wqkv, d_bqkv, d_wout, d_bout

    return jax.shard_map(
        local_block, mesh=grid_mesh,
        in_specs=(tok_spec, tok_spec, P(), P(), P(), P(), P(), P(), P()),
        out_specs=(tok_spec, tok_spec, P(), P(), P(), P(), P(), P()), check_vma=False)
```
